128 devices in a mesh: gx: 8 (over z, core), gy: 16 (over y, x).
Axes of the slice: x: 4, y: 4, z: 4, core: 2. Of those that a mesh axis runs over, the one named last changes fastest.
Arguments:
- tables: float32 [2, 1048576, 128], P(None, ('gx', 'gy')), may hold values from -0.9 to 0.9
- cold_rows: int32 [128, 2, 128, 16], P(('gx', 'gy')), may hold values from 0 to 8191, as said below
- cold_bags: int32 [128, 2, 128, 16], P(('gx', 'gy')), may hold values from -1 to 127, as said below
- hot_rows: int32 [2, 256], replicated, may hold values from 0 to 1048575
- hot_ids: int32 [16384, 2, 8], P(('gx', 'gy')), may hold values from 0 to 255
Outputs:
- pooled: float32 [16384, 2, 128], P(('gx', 'gy'))
The draws below stay inside these ranges and needn't reach their ends.
Inputs may be any that keep to these rules, and one draw needn't show every extreme that they name: `cold_rows`: every entry names one of the owner's 8192 rows. `cold_bags`: live slots of one sender, table and owner come first, the empty ones (-1) after them; in every draw each table has an owner whose 16 slots are all live from every sender.
All inputs are finite; a program needn't handle non-finite values.
Results may differ from the reference program's by a relative error of at most 0.0003.
Values sent between devices are 32-bit elements; how exact they have to be, the bound alone decides.
A program may use at most 64 MiB of HBM per device.

```python
import jax
import jax.numpy as jnp
from jax import lax

DIM = 128
ROWS_DEV = 8192
TABLES = 2
BATCH_DEV = 128
CAP = 16
HOT = 256
HOT_BAG = 8
PEERS = 128
BATCH = 16384
ROWS = 1048576


def draw_cold_rows(key, part):
    shape_all = (PEERS, TABLES, PEERS, CAP)
    exponent = jax.random.randint(jax.random.fold_in(key, 101), shape_all, 0, 21)
    limit = jnp.minimum(jnp.left_shift(jnp.ones(shape_all, jnp.int32), exponent), ROWS_DEV)
    return jax.random.randint(jax.random.fold_in(key, 102), shape_all, 0, limit).astype(jnp.int32)


def draw_cold_bags(key, part):
    shape_all = (PEERS, TABLES, PEERS, CAP)
    busiest = jax.random.randint(jax.random.fold_in(key, 201), (TABLES,), 0, PEERS)
    filled = jax.random.randint(jax.random.fold_in(key, 202), (PEERS, TABLES, PEERS), max(1, CAP // 4), CAP + 1)
    owner_index = jnp.arange(PEERS, dtype=jnp.int32)[None, None, :]
    filled = jnp.where(owner_index == busiest[None, :, None], CAP, filled)
    samples = jax.random.randint(jax.random.fold_in(key, 203), shape_all, 0, BATCH_DEV)
    slot_index = jnp.arange(CAP, dtype=jnp.int32)
    return jnp.where(slot_index < filled[..., None], samples, -1).astype(jnp.int32)


def place_ends(entries, rng, smallest, largest):
    longest = entries.shape.index(max(entries.shape))
    spots = []
    for shift in (0, 1):
        where = [jax.random.randint(jax.random.fold_in(rng, axis), (), 0, length) for axis, length in enumerate(entries.shape)]
        where[longest] = (where[longest] + shift) % entries.shape[longest]
        spots.append(tuple(where))
    return entries.at[spots[0]].set(smallest).at[spots[1]].set(largest)


def shard_levels(own_key, extent, pieces, least, high):
    def one(position, parts):
        draws = jax.random.uniform(jax.random.fold_in(jax.random.fold_in(own_key, 6), position), (parts,), jnp.float32, least / len(pieces), high / len(pieces))
        return jnp.repeat(jnp.exp(draws), extent[position] // parts).reshape((-1,) + (1,) * (len(extent) - position - 1))

    gain = one(*pieces[0])
    for cut in pieces[1:]:
        gain = gain * one(*cut)
    return gain


def centred(stream_key, shape, deviation, reach, cuts=(), kind=jnp.bfloat16):
    drawn = jax.random.normal(stream_key, shape, jnp.float32) * deviation
    if len(cuts) > 0:
        drawn = shard_levels(stream_key, shape, cuts, -0.22, 0.18) * drawn
    return jnp.clip(drawn, min=-reach, max=reach).astype(kind)


def setup_inputs(seed: int = 0) -> dict:
    key_list = jax.random.split(jax.random.key(seed), 6)
    return {
        "tables": centred(key_list[0], (TABLES, ROWS, DIM), 0.15, 0.9, ((1, 128),), jnp.float32),
        "cold_rows": draw_cold_rows(jax.random.fold_in(key_list[5], 71), 0),
        "cold_bags": draw_cold_bags(jax.random.fold_in(key_list[5], 71), 0),
        "hot_rows": place_ends(jax.random.randint(key_list[3], (TABLES, HOT), 0, ROWS), jax.random.fold_in(key_list[3], 1), 0, ROWS - 1).astype(jnp.int32),
        "hot_ids": place_ends(jax.random.randint(key_list[4], (BATCH, TABLES, HOT_BAG), 0, HOT), jax.random.fold_in(key_list[4], 1), 0, HOT - 1).astype(jnp.int32),
    }


def take_rows(matrix, indices):
    return jnp.take(matrix, indices, axis=0)


def reference(tables, cold_rows, cold_bags, hot_rows, hot_ids):
    offsets = (jnp.arange(PEERS, dtype=jnp.int32) * ROWS_DEV)[:, None]

    def per_table(table_index):
        one_table = tables[table_index]

        def per_sender(sender):
            slot_rows = (cold_rows[sender, table_index] + offsets).reshape(-1)
            slot_bags = cold_bags[sender, table_index].reshape(-1)
            looked = take_rows(one_table, slot_rows)
            live_mask = slot_bags >= 0
            segment = jnp.where(live_mask, slot_bags, 0).astype(jnp.int32)
            values = jnp.where(live_mask[:, None], looked, jnp.zeros_like(looked))
            return jax.ops.segment_sum(values, segment, num_segments=BATCH_DEV)

        return lax.map(per_sender, jnp.arange(PEERS, dtype=jnp.int32))

    cold_part = lax.map(per_table, jnp.arange(TABLES, dtype=jnp.int32))
    cold_part = jnp.transpose(cold_part, (1, 2, 0, 3)).reshape(BATCH, TABLES, DIM)
    hot_table = jax.vmap(take_rows)(tables, hot_rows)

    def pool_hot(table_rows, lookups):
        return jnp.sum(take_rows(table_rows, lookups), axis=1)

    hot_part = jax.vmap(pool_hot, in_axes=(0, 1), out_axes=1)(hot_table, hot_ids)
    return cold_part + hot_part
```

```python
import functools

import jax
import jax.numpy as jnp
from jax import lax
from jax.experimental import pallas as pl
from jax.experimental.pallas import tpu as pltpu
from jax.sharding import PartitionSpec as P

MESH = pl.DeviceIdType.MESH
GX, GY = 8, 16
PEERS = GX * GY
CAP, TABLES, DIM = 16, 2, 128
ROWS_DEV, HOT, HOT_BAG, BATCH_DEV = 8192, 256, 8, 128
SLOTS = TABLES * CAP
STEP = 37


def split_bf16(x):
    high = x.astype(jnp.bfloat16)
    low = (x - high.astype(jnp.float32)).astype(jnp.bfloat16)
    return high, low


def kernel(
    tab_hbm, rows_hbm, bags_hbm, hot_rows_hbm, hot_ids_hbm, out_ref,
    tab, rows_v, bags_v, hot_rows_s, hot_ids_v, msg_t, idx_out, idx_in,
    bags_t, lanes, sbuf, rbuf, hot_own, hot_r1, hot_s1, hot_r2, hot_s2, hot_mine, hot_all, hot_flat,
    tab_sem, in_sems, idx_ssem, idx_rsem, self_sem, row_ssem, row_rsem,
    h_ssem, h_rsem,
):
    gx, gy = lax.axis_index("gx"), lax.axis_index("gy")
    me = gx * GY + gy
    z, core, y, x = gx // 2, gx % 2, gy // 4, gy % 4

    def peer(k):
        q = lax.rem(k * STEP, PEERS)
        px = lax.rem(z + q // 32, 4) * 2 + lax.rem(core + lax.rem(q // 16, 2), 2)
        py = lax.rem(y + lax.rem(q // 4, 4), 4) * 4 + lax.rem(x + lax.rem(q, 4), 4)
        return px, py

    barrier = pltpu.get_barrier_semaphore()

    def greet(k, carry):
        pl.semaphore_signal(barrier, inc=1, device_id=peer(k), device_id_type=MESH)
        return carry

    lax.fori_loop(1, PEERS, greet, 0)

    small = [
        pltpu.make_async_copy(rows_hbm, rows_v, in_sems.at[0]),
        pltpu.make_async_copy(hot_rows_hbm, hot_rows_s, in_sems.at[1]),
        pltpu.make_async_copy(bags_hbm, bags_v, in_sems.at[2]),
        pltpu.make_async_copy(hot_ids_hbm, hot_ids_v, in_sems.at[3]),
    ]
    for copy in small:
        copy.start()
    table_copy = pltpu.make_async_copy(tab_hbm, tab, tab_sem)
    table_copy.start()

    small[0].wait()
    padded = jnp.concatenate(
        [rows_v[...], jnp.zeros((PEERS - SLOTS, PEERS), jnp.int32)], axis=0
    )
    msg_t[...] = padded.T
    for p in range(PEERS):
        idx_out[p] = msg_t[pl.ds(p, 1), :]
    own_idx = pltpu.make_async_copy(idx_out.at[me], idx_in.at[me], self_sem)
    own_idx.start()

    small[1].wait()
    table_copy.wait()
    first = me * ROWS_DEV
    for t in range(TABLES):

        def pick_hot(i, carry, t=t):
            for j in range(4):
                local = hot_rows_s[t, i * 4 + j] - first
                mine = jnp.logical_and(local >= 0, local < ROWS_DEV)
                at = jnp.where(mine, local, 0)
                scale = jnp.where(mine, 1.0, 0.0)
                row = tab[t * ROWS_DEV + at]
                hot_own[t * 4 + i // 16, lax.rem(i, 16), pl.ds(j, 1), :] = row * scale
            return carry

        lax.fori_loop(0, HOT // 4, pick_hot, 0)

    pl.semaphore_wait(barrier, PEERS - 1)

    def send_idx(k, carry):
        px, py = peer(k)
        pltpu.make_async_remote_copy(
            src_ref=idx_out.at[px * GY + py], dst_ref=idx_in.at[me],
            send_sem=idx_ssem, recv_sem=idx_rsem.at[me],
            device_id=(px, py), device_id_type=MESH,
        ).start()
        return carry

    lax.fori_loop(1, PEERS, send_idx, 0)

    def gx_peer(k):
        return lax.rem(gx + k, GX)

    def gy_peer(k):
        return lax.rem(gy + k, GY)

    def hot_send(src, dst, stage, slot, device):
        pltpu.make_async_remote_copy(
            src_ref=src, dst_ref=dst, send_sem=h_ssem.at[stage], recv_sem=h_rsem.at[stage],
            device_id=device, device_id_type=MESH,
        ).start()

    def h_stage1(k, carry):
        d = gx_peer(k)
        hot_send(hot_own.at[d], hot_r1.at[k - 1], 0, 0, (d, gy))
        return carry

    lax.fori_loop(1, GX, h_stage1, 0)

    def drain(ref, sem):
        pltpu.make_async_copy(ref, ref, sem).wait()

    drain(hot_r1, h_rsem.at[0])
    total = hot_own[gx]
    for k in range(GX - 1):
        total = total + hot_r1[k]
    hot_s1[...] = total

    def h_stage2(k, carry):
        d = gy_peer(k)
        hot_send(hot_s1.at[d], hot_r2.at[k - 1], 1, 0, (gx, d))
        return carry

    lax.fori_loop(1, GY, h_stage2, 0)

    def fetch(p, put):
        for t in range(TABLES):
            for c in range(CAP):
                put(t * CAP + c, tab[t * ROWS_DEV + idx_in[p, 0, t * CAP + c]])

    def serve(k, carry):
        px, py = peer(k)
        p = px * GY + py
        drain(idx_in.at[p], idx_rsem.at[p])

        def put(slot, row):
            sbuf[k, pl.ds(slot, 1), :] = row

        fetch(p, put)
        pltpu.make_async_remote_copy(
            src_ref=sbuf.at[k], dst_ref=rbuf.at[me],
            send_sem=row_ssem, recv_sem=row_rsem,
            device_id=(px, py), device_id_type=MESH,
        ).start()
        return carry

    lax.fori_loop(1, 32, serve, 0)

    drain(hot_r2, h_rsem.at[1])
    total2 = hot_s1[gy]
    for k in range(GY - 1):
        total2 = total2 + hot_r2[k]
    hot_s2[...] = total2
    hot_mine[gy] = total2

    def h_stage3(k, carry):
        hot_send(hot_s2, hot_mine.at[gy], 2, 0, (gx, gy_peer(k)))
        return carry

    lax.fori_loop(1, GY, h_stage3, 0)

    lax.fori_loop(32, 64, serve, 0)

    drain(hot_r2, h_rsem.at[2])

    def h_stage4(k, carry):
        hot_send(hot_mine, hot_all.at[gx], 3, 0, (gx_peer(k), gy))
        return carry

    lax.fori_loop(1, GX, h_stage4, 0)
    hot_all[gx] = hot_mine[...]

    lax.fori_loop(64, PEERS, serve, 0)

    own_idx.wait()

    def put_own(slot, row):
        rbuf[me, pl.ds(slot, 1), :] = row

    fetch(me, put_own)

    small[2].wait()
    bags_t[...] = jnp.concatenate(
        [bags_v[...], jnp.zeros((PEERS - SLOTS, PEERS), jnp.int32)], axis=0
    ).T
    lane = lax.broadcasted_iota(jnp.int32, (CAP, PEERS), 1)
    for t in range(TABLES):
        line = jnp.zeros((CAP, PEERS), jnp.int32)
        for j in range(8):
            part = bags_t[pl.ds(j, 16, stride=8), :]
            moved = pltpu.roll(part, (j * CAP - t * CAP) % PEERS, axis=1)
            line = jnp.where(lane // CAP == j, moved, line)
        lanes[t] = line

    small[3].wait()
    drain(hot_r1, h_rsem.at[3])
    for b in range(GX):
        for g in range(GY):
            hot_flat[pl.ds((b * GY + g) * 4, 4), :] = hot_all[b, g]
    spot = lax.broadcasted_iota(jnp.int32, (HOT, BATCH_DEV), 0)
    sample = lax.broadcasted_iota(jnp.int32, (BATCH_DEV, 2 * PEERS), 0)
    parts = []
    for t in range(TABLES):
        counts = jnp.zeros((HOT, BATCH_DEV), jnp.float32)
        for k in range(HOT_BAG):
            ids = hot_ids_v[pl.ds(t * HOT_BAG + k, 1), :]
            counts = counts + jnp.where(ids == spot, 1.0, 0.0)
        counts = counts.T.astype(jnp.bfloat16)
        high, low = split_bf16(hot_flat[pl.ds(t * HOT, HOT), :])
        both = jnp.concatenate([high, low], axis=1)
        parts.append(jnp.dot(counts, both, preferred_element_type=jnp.float32))

    pltpu.make_async_copy(rbuf.at[pl.ds(0, PEERS - 1)], rbuf.at[pl.ds(0, PEERS - 1)], row_rsem).wait()
    for t in range(TABLES):
        acc = parts[t]
        for q in range(8):
            wanted = jnp.concatenate(
                [lanes[t, pl.ds(2 * q, 1), :], lanes[t, pl.ds(2 * q + 1, 1), :]], axis=1
            )
            onehot = jnp.where(wanted == sample, 1.0, 0.0).astype(jnp.bfloat16)
            rows = rbuf[pl.ds(q * 16, 16), pl.ds(t * CAP, CAP), :].reshape(256, DIM)
            high, low = split_bf16(rows)
            both = jnp.concatenate([high, low], axis=1)
            acc = acc + jnp.dot(onehot, both, preferred_element_type=jnp.float32)
        out_ref[pl.ds(t, BATCH_DEV, stride=2), :] = acc[:, :DIM] + acc[:, DIM:]

    drain(idx_out.at[pl.ds(0, PEERS - 1)], idx_ssem)
    drain(sbuf.at[pl.ds(0, PEERS - 1)], row_ssem)
    drain(hot_r1, h_ssem.at[0])
    drain(hot_r2, h_ssem.at[1])
    drain(hot_r2, h_ssem.at[2])
    drain(hot_r1, h_ssem.at[3])


def body(tables, cold_rows, cold_bags, hot_rows, hot_ids):
    tab = tables.reshape(TABLES * ROWS_DEV, 1, DIM)
    rows = cold_rows[0].transpose(0, 2, 1).reshape(SLOTS, PEERS)
    bags = cold_bags[0].transpose(0, 2, 1).reshape(SLOTS, PEERS)
    ids = hot_ids.transpose(1, 2, 0).reshape(TABLES * HOT_BAG, BATCH_DEV)
    f32, i32 = jnp.float32, jnp.int32
    out = pl.pallas_call(
        kernel,
        out_shape=jax.ShapeDtypeStruct((BATCH_DEV * TABLES, DIM), f32),
        in_specs=[pl.BlockSpec(memory_space=pl.ANY)] * 5,
        out_specs=pl.BlockSpec(memory_space=pltpu.VMEM),
        scratch_shapes=[
            pltpu.VMEM((TABLES * ROWS_DEV, 1, DIM), f32),
            pltpu.VMEM((SLOTS, PEERS), i32),
            pltpu.VMEM((SLOTS, PEERS), i32),
            pltpu.SMEM((TABLES, HOT), i32),
            pltpu.VMEM((TABLES * HOT_BAG, BATCH_DEV), i32),
            pltpu.VMEM((PEERS, PEERS), i32),
            pltpu.VMEM((PEERS, 1, PEERS), i32),
            pltpu.SMEM((PEERS, 1, PEERS), i32),
            pltpu.VMEM((PEERS, PEERS), i32),
            pltpu.VMEM((TABLES, CAP, PEERS), i32),
            pltpu.VMEM((PEERS, SLOTS, DIM), f32),
            pltpu.VMEM((PEERS, SLOTS, DIM), f32),
            pltpu.VMEM((GX, GY, 4, DIM), f32),
            pltpu.VMEM((GX - 1, GY, 4, DIM), f32),
            pltpu.VMEM((GY, 4, DIM), f32),
            pltpu.VMEM((GY - 1, 4, DIM), f32),
            pltpu.VMEM((4, DIM), f32),
            pltpu.VMEM((GY, 4, DIM), f32),
            pltpu.VMEM((GX, GY, 4, DIM), f32),
            pltpu.VMEM((TABLES * HOT, DIM), f32),
            pltpu.SemaphoreType.DMA,
            pltpu.SemaphoreType.DMA((4,)),
            pltpu.SemaphoreType.DMA,
            pltpu.SemaphoreType.DMA((PEERS,)),
            pltpu.SemaphoreType.DMA,
            pltpu.SemaphoreType.DMA,
            pltpu.SemaphoreType.DMA,
            pltpu.SemaphoreType.DMA((4,)),
            pltpu.SemaphoreType.DMA((4,)),
        ],
        compiler_params=pltpu.CompilerParams(
            collective_id=0, has_side_effects=True, vmem_limit_bytes=48 << 20
        ),
    )(tab, rows, bags, hot_rows, ids)
    return out.reshape(BATCH_DEV, TABLES, DIM)


def solution(mesh):
    both = ("gx", "gy")
    return jax.shard_map(
        body,
        mesh=mesh,
        in_specs=(
            P(None, both, None),
            P(both, None, None, None),
            P(both, None, None, None),
            P(),
            P(both, None, None),
        ),
        out_specs=P(both, None, None),
        check_vma=False,
    )
```

```python
import jax
import jax.numpy as jnp
from jax import lax
from jax.experimental import pallas as pl
from jax.experimental.pallas import tpu as pltpu
from jax.sharding import PartitionSpec as P

MESH = pl.DeviceIdType.MESH
GX, GY = 8, 16
PEERS = GX * GY
CAP, TABLES, DIM = 16, 2, 128
ROWS_DEV, HOT, HOT_BAG, BATCH_DEV = 8192, 256, 8, 128
SLOTS = TABLES * CAP
ORDER = [
    (0, 0), (0, 1), (0, 3), (1, 0), (3, 0), (1, 1), (3, 3), (0, 2), (2, 0),
    (1, 3), (3, 1), (2, 2), (1, 2), (2, 3), (3, 2), (2, 1),
]


def split_bf16(x):
    high = x.astype(jnp.bfloat16)
    low = (x - high.astype(jnp.float32)).astype(jnp.bfloat16)
    return high, low


def kernel(
    tab_hbm, rows_hbm, bags_hbm, hot_rows_hbm, hot_ids_hbm, out_ref,
    tab, rows_v, bags_v, hot_rows_v, hot_at_v, hot_at, hot_ids_v, msg_t, idx_out, idx_mid, idx_in,
    bags_t, lanes, sbuf, rbuf, hot_own, hot_r1, hot_s1, hot_r2, hot_s2, hot_mine, hot_all, hot_flat,
    tab_sem, in_sems, at_sem, idx_ssem1, idx_rsem1, idx_ssem2, idx_rsem2, self_sem,
    row_ssem, row_rsem, h_ssem, h_rsem,
):
    gx, gy = lax.axis_index("gx"), lax.axis_index("gy")
    me = gx * GY + gy
    y, x = gy // 4, lax.rem(gy, 4)

    def gx_peer(k):
        return lax.rem(gx + k, GX)

    def gy_peer(dy, dx):
        return lax.rem(y + dy, 4) * 4 + lax.rem(x + dx, 4)

    cross = [gy_peer(dy, dx) for dy, dx in ORDER]
    ring = [gx_peer(k) for k in range(1, GX)]

    small = [
        pltpu.make_async_copy(rows_hbm, rows_v, in_sems.at[0]),
        pltpu.make_async_copy(hot_rows_hbm, hot_rows_v, in_sems.at[1]),
        pltpu.make_async_copy(bags_hbm, bags_v, in_sems.at[2]),
        pltpu.make_async_copy(hot_ids_hbm, hot_ids_v, in_sems.at[3]),
    ]
    small[0].start()

    barrier = pltpu.get_barrier_semaphore()
    for d in ring:
        pl.semaphore_signal(barrier, inc=1, device_id=(d, gy), device_id_type=MESH)
    for d in cross[1:]:
        pl.semaphore_signal(barrier, inc=1, device_id=(gx, d), device_id_type=MESH)

    for copy in small[1:]:
        copy.start()
    piece = TABLES * ROWS_DEV // 8
    for i in range(8):
        part = pl.ds(i * piece, piece)
        pltpu.make_async_copy(tab_hbm.at[part], tab.at[part], tab_sem).start()
    tab[TABLES * ROWS_DEV] = jnp.zeros((1, DIM), jnp.float32)

    small[1].wait()
    local = hot_rows_v[...] - me * ROWS_DEV
    mine = jnp.logical_and(local >= 0, local < ROWS_DEV)
    table = lax.broadcasted_iota(jnp.int32, (TABLES, HOT), 0)
    hot_at_v[...] = jnp.where(mine, local + table * ROWS_DEV, TABLES * ROWS_DEV)
    at_copy = pltpu.make_async_copy(hot_at_v, hot_at, at_sem)
    at_copy.start()

    small[0].wait()
    slot = lax.broadcasted_iota(jnp.int32, (SLOTS, PEERS), 0)
    padded = jnp.concatenate(
        [
            rows_v[...] + jnp.where(slot < CAP, 0, ROWS_DEV),
            jnp.zeros((PEERS - SLOTS, PEERS), jnp.int32),
        ],
        axis=0,
    )
    msg_t[...] = padded.T
    for p in range(PEERS):
        idx_out[p // GY, p % GY] = msg_t[pl.ds(p, 1), :]
    for g in range(GY):
        idx_mid[g, gx] = idx_out[gx, g]

    pl.semaphore_wait(barrier, GX + GY - 2)

    for d in ring:
        pltpu.make_async_remote_copy(
            src_ref=idx_out.at[d], dst_ref=idx_mid.at[:, gx],
            send_sem=idx_ssem1, recv_sem=idx_rsem1,
            device_id=(d, gy), device_id_type=MESH,
        ).start()

    def drain(ref, sem):
        pltpu.make_async_copy(ref, ref, sem).wait()

    def hot_send(src, dst, stage, device):
        pltpu.make_async_remote_copy(
            src_ref=src, dst_ref=dst, send_sem=h_ssem.at[stage], recv_sem=h_rsem.at[stage],
            device_id=device, device_id_type=MESH,
        ).start()

    at_copy.wait()
    drain(tab.at[pl.ds(0, TABLES * ROWS_DEV)], tab_sem)

    def pick_hot(i, carry):
        t, rest = i // GY, lax.rem(i, GY) * 16
        for j in range(16):
            row = tab[hot_at[t, rest + j]]
            hot_own[i // 4, lax.rem(i, 4) * 4 + j // 4, pl.ds(j % 4, 1), :] = row
        return carry

    lax.fori_loop(0, TABLES * HOT // 16, pick_hot, 0)
    for k, d in enumerate(ring):
        hot_send(hot_own.at[d], hot_r1.at[k], 0, (d, gy))

    drain(idx_mid.at[pl.ds(0, 14)], idx_rsem1)
    for d in cross[1:]:
        pltpu.make_async_remote_copy(
            src_ref=idx_mid.at[d], dst_ref=idx_in.at[gy],
            send_sem=idx_ssem2, recv_sem=idx_rsem2.at[gy],
            device_id=(gx, d), device_id_type=MESH,
        ).start()
    own_idx = pltpu.make_async_copy(idx_mid.at[gy], idx_in.at[gy], self_sem)
    own_idx.start()

    drain(hot_r1, h_rsem.at[0])
    total = hot_own[gx]
    for k in range(GX - 1):
        total = total + hot_r1[k]
    hot_s1[...] = total
    for k, d in enumerate(cross[1:]):
        hot_send(hot_s1.at[d], hot_r2.at[k], 1, (gx, d))

    def fetch(g, j, put):
        for slot in range(SLOTS):
            put(slot, tab[idx_in[g, j, 0, slot]])

    def serve(g, n):
        if n:
            drain(idx_in.at[g], idx_rsem2.at[g])
        else:
            own_idx.wait()

        def one(k, carry):
            d = gx_peer(k)

            def put(slot, row):
                sbuf[n * GX + k, pl.ds(slot, 1), :] = row

            fetch(g, d, put)
            pltpu.make_async_remote_copy(
                src_ref=sbuf.at[n * GX + k], dst_ref=rbuf.at[me],
                send_sem=row_ssem, recv_sem=row_rsem,
                device_id=(d, g), device_id_type=MESH,
            ).start()
            return carry

        lax.fori_loop(0 if n else 1, GX, one, 0)

    for n in range(0, 5):
        serve(cross[n], n)

    drain(hot_r2, h_rsem.at[1])
    total2 = hot_s1[gy]
    for k in range(GY - 1):
        total2 = total2 + hot_r2[k]
    hot_s2[...] = total2
    hot_mine[gy] = total2
    for d in cross[1:]:
        hot_send(hot_s2, hot_mine.at[gy], 2, (gx, d))

    for n in range(5, 10):
        serve(cross[n], n)

    drain(hot_r2, h_rsem.at[2])
    for d in ring:
        hot_send(hot_mine, hot_all.at[gx], 3, (d, gy))
    hot_all[gx] = hot_mine[...]

    for n in range(10, GY):
        serve(cross[n], n)

    def put_own(slot, row):
        rbuf[me, pl.ds(slot, 1), :] = row

    fetch(gy, gx, put_own)

    small[2].wait()
    bags_t[...] = jnp.concatenate(
        [bags_v[...], jnp.zeros((PEERS - SLOTS, PEERS), jnp.int32)], axis=0
    ).T
    lane = lax.broadcasted_iota(jnp.int32, (CAP, PEERS), 1)
    for t in range(TABLES):
        line = jnp.zeros((CAP, PEERS), jnp.int32)
        for j in range(8):
            part = bags_t[pl.ds(j, 16, stride=8), :]
            moved = pltpu.roll(part, (j * CAP - t * CAP) % PEERS, axis=1)
            line = jnp.where(lane // CAP == j, moved, line)
        lanes[t] = line

    small[3].wait()
    drain(hot_r1, h_rsem.at[3])
    for b in range(GX):
        for g in range(GY):
            hot_flat[pl.ds((b * GY + g) * 4, 4), :] = hot_all[b, g]
    spot = lax.broadcasted_iota(jnp.int32, (HOT, BATCH_DEV), 0)
    sample = lax.broadcasted_iota(jnp.int32, (BATCH_DEV, 2 * PEERS), 0)
    parts = []
    for t in range(TABLES):
        counts = jnp.zeros((HOT, BATCH_DEV), jnp.float32)
        for k in range(HOT_BAG):
            ids = hot_ids_v[pl.ds(t * HOT_BAG + k, 1), :]
            counts = counts + jnp.where(ids == spot, 1.0, 0.0)
        counts = counts.T.astype(jnp.bfloat16)
        high, low = split_bf16(hot_flat[pl.ds(t * HOT, HOT), :])
        both = jnp.concatenate([high, low], axis=1)
        parts.append(jnp.dot(counts, both, preferred_element_type=jnp.float32))

    drain(rbuf.at[pl.ds(0, PEERS - 1)], row_rsem)
    for t in range(TABLES):
        acc = parts[t]
        for q in range(8):
            wanted = jnp.concatenate(
                [lanes[t, pl.ds(2 * q, 1), :], lanes[t, pl.ds(2 * q + 1, 1), :]], axis=1
            )
            onehot = jnp.where(wanted == sample, 1.0, 0.0).astype(jnp.bfloat16)
            rows = rbuf[pl.ds(q * 16, 16), pl.ds(t * CAP, CAP), :].reshape(256, DIM)
            high, low = split_bf16(rows)
            both = jnp.concatenate([high, low], axis=1)
            acc = acc + jnp.dot(onehot, both, preferred_element_type=jnp.float32)
        out_ref[pl.ds(t, BATCH_DEV, stride=2), :] = acc[:, :DIM] + acc[:, DIM:]

    drain(idx_mid.at[pl.ds(0, 14)], idx_ssem1)
    drain(idx_mid.at[pl.ds(0, 15)], idx_ssem2)
    drain(sbuf.at[pl.ds(0, PEERS - 1)], row_ssem)
    drain(hot_r1, h_ssem.at[0])
    drain(hot_r2, h_ssem.at[1])
    drain(hot_r2, h_ssem.at[2])
    drain(hot_r1, h_ssem.at[3])


def body(tables, cold_rows, cold_bags, hot_rows, hot_ids):
    tab = tables.reshape(TABLES * ROWS_DEV, 1, DIM)
    rows = cold_rows[0].transpose(0, 2, 1).reshape(SLOTS, PEERS)
    bags = cold_bags[0].transpose(0, 2, 1).reshape(SLOTS, PEERS)
    ids = hot_ids.transpose(1, 2, 0).reshape(TABLES * HOT_BAG, BATCH_DEV)
    f32, i32 = jnp.float32, jnp.int32
    out = pl.pallas_call(
        kernel,
        out_shape=jax.ShapeDtypeStruct((BATCH_DEV * TABLES, DIM), f32),
        in_specs=[pl.BlockSpec(memory_space=pltpu.MemorySpace.HBM)] * 5,
        out_specs=pl.BlockSpec(memory_space=pltpu.VMEM),
        scratch_shapes=[
            pltpu.VMEM((TABLES * ROWS_DEV + 1, 1, DIM), f32),
            pltpu.VMEM((SLOTS, PEERS), i32),
            pltpu.VMEM((SLOTS, PEERS), i32),
            pltpu.VMEM((TABLES, HOT), i32),
            pltpu.VMEM((TABLES, HOT), i32),
            pltpu.SMEM((TABLES, HOT), i32),
            pltpu.VMEM((TABLES * HOT_BAG, BATCH_DEV), i32),
            pltpu.VMEM((PEERS, PEERS), i32),
            pltpu.VMEM((GX, GY, 1, PEERS), i32),
            pltpu.VMEM((GY, GX, 1, PEERS), i32),
            pltpu.SMEM((GY, GX, 1, PEERS), i32),
            pltpu.VMEM((PEERS, PEERS), i32),
            pltpu.VMEM((TABLES, CAP, PEERS), i32),
            pltpu.VMEM((PEERS, SLOTS, DIM), f32),
            pltpu.VMEM((PEERS, SLOTS, DIM), f32),
            pltpu.VMEM((GX, GY, 4, DIM), f32),
            pltpu.VMEM((GX - 1, GY, 4, DIM), f32),
            pltpu.VMEM((GY, 4, DIM), f32),
            pltpu.VMEM((GY - 1, 4, DIM), f32),
            pltpu.VMEM((4, DIM), f32),
            pltpu.VMEM((GY, 4, DIM), f32),
            pltpu.VMEM((GX, GY, 4, DIM), f32),
            pltpu.VMEM((TABLES * HOT, DIM), f32),
            pltpu.SemaphoreType.DMA,
            pltpu.SemaphoreType.DMA((4,)),
            pltpu.SemaphoreType.DMA,
            pltpu.SemaphoreType.DMA,
            pltpu.SemaphoreType.DMA,
            pltpu.SemaphoreType.DMA,
            pltpu.SemaphoreType.DMA((GY,)),
            pltpu.SemaphoreType.DMA,
            pltpu.SemaphoreType.DMA,
            pltpu.SemaphoreType.DMA,
            pltpu.SemaphoreType.DMA((4,)),
            pltpu.SemaphoreType.DMA((4,)),
        ],
        compiler_params=pltpu.CompilerParams(
            collective_id=0, has_side_effects=True, vmem_limit_bytes=48 << 20
        ),
    )(tab, rows, bags, hot_rows, ids)
    return out.reshape(BATCH_DEV, TABLES, DIM)


def solution(mesh):
    both = ("gx", "gy")
    return jax.shard_map(
        body,
        mesh=mesh,
        in_specs=(
            P(None, both, None),
            P(both, None, None, None),
            P(both, None, None, None),
            P(),
            P(both, None, None),
        ),
        out_specs=P(both, None, None),
        check_vma=False,
    )
```

```python
import jax
import jax.numpy as jnp
from jax import lax
from jax.experimental import pallas as pl
from jax.experimental.pallas import tpu as pltpu
from jax.sharding import PartitionSpec as P

MESH = pl.DeviceIdType.MESH
HBM = pltpu.MemorySpace.HBM
GX, GY = 8, 16
PEERS = GX * GY
CAP, TABLES, DIM = 16, 2, 128
ROWS_DEV, HOT, HOT_BAG, BATCH_DEV = 8192, 256, 8, 128
SLOTS = TABLES * CAP
STEP = 25
GROUP = 32
NEAR = 42
CORNERS = 54
CUTS = (6, 18)


def split_bf16(x):
    high = x.astype(jnp.bfloat16)
    low = (x - high.astype(jnp.float32)).astype(jnp.bfloat16)
    return high, low


def kernel(
    tab_hbm, rows_hbm, bags_hbm, hot_rows_hbm, hot_ids_hbm, out_ref,
    tab, rows_v, bags_v, hot_rows_v, hot_at_v, hot_at, hot_ids_v, msg_t, idx_out, idx_mid, idx_in, idx_near,
    bags_t, lanes, sbuf, rbuf, hot_own, hot_r0, hot_s0, hot_r1, hot_s1, hot_r2, hot_s2, hot_all,
    tab_sem, in_sems, at_sem, idx_ssem1, idx_rsem1, idx_ssem2, idx_rsem2, idx_csem, idx_crsem, self_sem,
    row_ssem, row_rsem, h_ssem, h_rsem,
):
    gx, gy = lax.axis_index("gx"), lax.axis_index("gy")
    me = gx * GY + gy
    y, x = gy // 4, lax.rem(gy, 4)
    z, core = gx // 2, lax.rem(gx, 2)

    def at(dz, dc, dy, dx):
        px = lax.rem(z + dz, 4) * 2 + lax.rem(core + dc, 2)
        return px, lax.rem(y + dy, 4) * 4 + lax.rem(x + dx, 4)

    group = [at(u // 8, u // 4 % 2, u % 4, 0) for u in range(1, GROUP)]
    near = [at(0, c // 4, c % 4, dx) for c in range(8) for dx in (1, 2, 3)]
    near += [at(dz, dc, 0, dx) for dz in (1, 2, 3) for dc in (0, 1) for dx in (1, 2, 3)]
    before = [at(dz, 0, dy, dx) for dz in (1, 2, 3) for dy in (1, 2, 3) for dx in (1, 3) if (dz + dy) % 2 != dx // 3]
    beside = [at(b // 4, 0, b % 4, 1 + (b + b // 4) % 2 * 2) for b in range(16)]
    along_x = [at(0, 0, 0, dx) for dx in (1, 2, 3)]

    def unit(px, py):
        return px * 4 + py // 4

    here = unit(gx, gy)
    block = z * 4 + y
    other = 1 - core
    partner = (z * 2 + other, gy)

    def drain(ref, sem):
        pltpu.make_async_copy(ref, ref, sem).wait()

    def hot_send(src, dst, stage, device):
        pltpu.make_async_remote_copy(
            src_ref=src, dst_ref=dst, send_sem=h_ssem.at[stage], recv_sem=h_rsem.at[stage],
            device_id=device, device_id_type=MESH,
        ).start()

    small = [
        pltpu.make_async_copy(rows_hbm, rows_v, in_sems.at[0]),
        pltpu.make_async_copy(hot_rows_hbm, hot_rows_v, in_sems.at[1]),
        pltpu.make_async_copy(bags_hbm, bags_v, in_sems.at[2]),
        pltpu.make_async_copy(hot_ids_hbm, hot_ids_v, in_sems.at[3]),
    ]
    for copy in small:
        copy.start()

    barrier = pltpu.get_barrier_semaphore()
    for device in before + near + group:
        pl.semaphore_signal(barrier, inc=1, device_id=device, device_id_type=MESH)
    tab[TABLES * ROWS_DEV] = jnp.zeros((1, DIM), jnp.float32)

    small[0].wait()
    piece = TABLES * ROWS_DEV // 8
    for i in range(8):
        part = pl.ds(i * piece, piece)
        pltpu.make_async_copy(tab_hbm.at[part], tab.at[part], tab_sem).start()
    slot = lax.broadcasted_iota(jnp.int32, (SLOTS, PEERS), 0)
    padded = jnp.concatenate(
        [
            rows_v[...] + jnp.where(slot < CAP, 0, ROWS_DEV),
            jnp.zeros((PEERS - SLOTS, PEERS), jnp.int32),
        ],
        axis=0,
    )
    msg_t[...] = padded.T
    for p in range(PEERS):
        idx_out[p] = msg_t[pl.ds(p, 1), :]
    for d in range(4):
        idx_mid[d, here] = idx_out[here * 4 + d]

    pl.semaphore_wait(barrier, len(before + near + group))

    for px, py in group:
        u = unit(px, py)
        pltpu.make_async_remote_copy(
            src_ref=idx_out.at[pl.ds(u * 4, 4)], dst_ref=idx_mid.at[:, here],
            send_sem=idx_ssem1, recv_sem=idx_rsem1,
            device_id=(px, py), device_id_type=MESH,
        ).start()
    for px, py in near:
        pltpu.make_async_remote_copy(
            src_ref=idx_out.at[px * GY + py], dst_ref=idx_near.at[me],
            send_sem=idx_csem, recv_sem=idx_crsem,
            device_id=(px, py), device_id_type=MESH,
        ).start()

    small[1].wait()
    local = hot_rows_v[...] - me * ROWS_DEV
    mine = jnp.logical_and(local >= 0, local < ROWS_DEV)
    table = lax.broadcasted_iota(jnp.int32, (TABLES, HOT), 0)
    hot_at_v[...] = jnp.where(mine, local + table * ROWS_DEV, TABLES * ROWS_DEV)
    at_copy = pltpu.make_async_copy(hot_at_v, hot_at, at_sem)
    at_copy.start()
    at_copy.wait()

    drain(tab.at[pl.ds(0, TABLES * ROWS_DEV)], tab_sem)

    def pick_hot(i, carry):
        t, block = i // 4, lax.rem(i, 4)
        for j in range(64):
            row = tab[hot_at[t, block * 64 + j]]
            hot_own[t, block * 4 + j // 16, pl.ds(j % 16, 1), :] = row
        return carry

    lax.fori_loop(0, TABLES * 4, pick_hot, 0)
    hot_send(hot_own.at[other], hot_r0, 0, partner)

    def serve(px, py, n, wanted):
        for slot in range(SLOTS):
            sbuf[n, pl.ds(slot, 1), :] = tab[wanted(px, py, slot)]
        pltpu.make_async_remote_copy(
            src_ref=sbuf.at[n], dst_ref=rbuf.at[me],
            send_sem=row_ssem, recv_sem=row_rsem,
            device_id=(px, py), device_id_type=MESH,
        ).start()

    def from_near(px, py, slot):
        return idx_near[px * GY + py, 0, slot]

    def from_far(px, py, slot):
        return idx_in[lax.rem(py, 4), unit(px, py), 0, slot]

    drain(hot_r0, h_rsem.at[0])
    hot_s0[...] = hot_own[core] + hot_r0[...]
    for px, py in beside:
        hot_send(hot_s0.at[px // 2 * 4 + py // 4], hot_r1.at[block], 1, (px, py))

    drain(idx_near.at[pl.ds(0, NEAR)], idx_crsem)
    for k, (c, dx) in enumerate([(6, 1), (7, 3), (6, 2), (7, 1), (6, 3), (7, 2)]):
        serve(*at(0, c // 4, c % 4, dx), 66 + k, from_near)

    pltpu.make_async_copy(idx_mid.at[:, pl.ds(0, GROUP - 1)], idx_mid.at[:, pl.ds(0, GROUP - 1)], idx_rsem1).wait()
    for device in along_x:
        pltpu.make_async_remote_copy(
            src_ref=idx_mid.at[lax.rem(device[1], 4)], dst_ref=idx_in.at[x],
            send_sem=idx_ssem2, recv_sem=idx_rsem2,
            device_id=device, device_id_type=MESH,
        ).start()
    own_idx = pltpu.make_async_copy(idx_mid.at[x], idx_in.at[x], self_sem)
    own_idx.start()

    own_idx.wait()

    def in_group(e):
        u = lax.rem(e * 11, GROUP)
        return at(u // 8, lax.rem(u // 4, 2), lax.rem(u, 4), 0)

    def serve_near(i, carry):
        n = i * 11
        for dx in (1, 2, 3):
            serve(*at(1 + i // 2, lax.rem(i, 2), 0, dx), n, from_near)
            serve(*at(0, i // 4, lax.rem(i, 4), 4 - dx), n + 1, from_near)
            serve(*in_group(i * 5 + dx), n + 2, from_far)
            n = n + 3
        serve(*in_group(i * 5 + 4), n, from_far)
        serve(*in_group(i * 5 + 5), n + 1, from_far)
        return carry

    lax.fori_loop(0, CUTS[0], serve_near, 0)

    drain(hot_r1, h_rsem.at[1])
    total = hot_r1[0]
    for k in range(1, 16):
        total = total + hot_r1[k]
    hot_s1[...] = total
    for k, device in enumerate(along_x):
        hot_send(hot_s1, hot_r2.at[k], 2, device)

    lax.fori_loop(CUTS[0], 6, serve_near, 0)
    serve(*in_group(31), 72, from_far)

    drain(idx_in.at[pl.ds(0, 3)], idx_rsem2)

    def serve_corner(k, carry):
        q = lax.rem(k * STEP, CORNERS)
        h = lax.rem(q, 9)
        device = at(1 + q // 18, lax.rem(q // 9, 2), 1 + h // 3, 1 + lax.rem(h, 3))
        serve(*device, PEERS - 1 - CORNERS + k, from_far)
        return carry

    lax.fori_loop(0, CUTS[1], serve_corner, 0)

    drain(hot_r2, h_rsem.at[2])
    total = (hot_s1[...] + hot_r2[0]) + (hot_r2[1] + hot_r2[2])
    hot_s2[...] = total
    hot_all[core, block] = total
    for device in beside[1:]:
        hot_send(hot_s2, hot_all.at[core, block], 3, device)

    lax.fori_loop(CUTS[1], CORNERS, serve_corner, 0)

    for slot in range(SLOTS):
        rbuf[me, pl.ds(slot, 1), :] = tab[idx_in[x, here, 0, slot]]

    small[2].wait()
    bags_t[...] = jnp.concatenate(
        [bags_v[...], jnp.zeros((PEERS - SLOTS, PEERS), jnp.int32)], axis=0
    ).T
    lane = lax.broadcasted_iota(jnp.int32, (CAP, PEERS), 1)
    for t in range(TABLES):
        line = jnp.zeros((CAP, PEERS), jnp.int32)
        for j in range(8):
            part = bags_t[pl.ds(j, 16, stride=8), :]
            moved = pltpu.roll(part, (j * CAP - t * CAP) % PEERS, axis=1)
            line = jnp.where(lane // CAP == j, moved, line)
        lanes[t] = line

    small[3].wait()
    drain(hot_r1.at[pl.ds(0, 15)], h_rsem.at[3])
    hot_send(hot_all.at[core], hot_all.at[core], 4, partner)

    drain(hot_r0, h_rsem.at[4])
    spot = lax.broadcasted_iota(jnp.int32, (HOT, BATCH_DEV), 0)
    sample = lax.broadcasted_iota(jnp.int32, (BATCH_DEV, 2 * PEERS), 0)
    parts = []
    for t in range(TABLES):
        counts = jnp.zeros((HOT, BATCH_DEV), jnp.float32)
        for k in range(HOT_BAG):
            ids = hot_ids_v[pl.ds(t * HOT_BAG + k, 1), :]
            counts = counts + jnp.where(ids == spot, 1.0, 0.0)
        counts = counts.T.astype(jnp.bfloat16)
        high, low = split_bf16(hot_all[t].reshape(HOT, DIM))
        both = jnp.concatenate([high, low], axis=1)
        parts.append(jnp.dot(counts, both, preferred_element_type=jnp.float32))

    drain(rbuf.at[pl.ds(0, PEERS - 1)], row_rsem)

    for t in range(TABLES):
        acc = parts[t]
        for q in range(8):
            wanted = jnp.concatenate(
                [lanes[t, pl.ds(2 * q, 1), :], lanes[t, pl.ds(2 * q + 1, 1), :]], axis=1
            )
            onehot = jnp.where(wanted == sample, 1.0, 0.0).astype(jnp.bfloat16)
            rows = rbuf[pl.ds(q * 16, 16), pl.ds(t * CAP, CAP), :].reshape(256, DIM)
            high, low = split_bf16(rows)
            both = jnp.concatenate([high, low], axis=1)
            acc = acc + jnp.dot(onehot, both, preferred_element_type=jnp.float32)
        out_ref[pl.ds(t, BATCH_DEV, stride=2), :] = acc[:, :DIM] + acc[:, DIM:]

    drain(idx_out.at[pl.ds(0, 4 * (GROUP - 1))], idx_ssem1)
    drain(idx_mid.at[pl.ds(0, 3)], idx_ssem2)
    drain(idx_near.at[pl.ds(0, NEAR)], idx_csem)
    drain(sbuf.at[pl.ds(0, PEERS - 1)], row_ssem)
    for stage, ref in enumerate((hot_r0, hot_r1, hot_r2, hot_r1.at[pl.ds(0, 15)], hot_r0)):
        drain(ref, h_ssem.at[stage])


def body(tables, cold_rows, cold_bags, hot_rows, hot_ids):
    tab = tables.reshape(TABLES * ROWS_DEV, 1, DIM)
    rows = cold_rows[0].transpose(0, 2, 1).reshape(SLOTS, PEERS)
    bags = cold_bags[0].transpose(0, 2, 1).reshape(SLOTS, PEERS)
    ids = hot_ids.transpose(1, 2, 0).reshape(TABLES * HOT_BAG, BATCH_DEV)
    f32, i32 = jnp.float32, jnp.int32
    out = pl.pallas_call(
        kernel,
        out_shape=jax.ShapeDtypeStruct((BATCH_DEV * TABLES, DIM), f32),
        in_specs=[pl.BlockSpec(memory_space=HBM)] * 5,
        out_specs=pl.BlockSpec(memory_space=pltpu.VMEM),
        scratch_shapes=[
            pltpu.VMEM((TABLES * ROWS_DEV + 1, 1, DIM), f32),
            pltpu.VMEM((SLOTS, PEERS), i32),
            pltpu.VMEM((SLOTS, PEERS), i32),
            pltpu.VMEM((TABLES, HOT), i32),
            pltpu.VMEM((TABLES, HOT), i32),
            pltpu.SMEM((TABLES, HOT), i32),
            pltpu.VMEM((TABLES * HOT_BAG, BATCH_DEV), i32),
            pltpu.VMEM((PEERS, PEERS), i32),
            pltpu.VMEM((PEERS, 1, PEERS), i32),
            pltpu.VMEM((4, GROUP, 1, PEERS), i32),
            pltpu.SMEM((4, GROUP, 1, PEERS), i32),
            pltpu.SMEM((PEERS, 1, PEERS), i32),
            pltpu.VMEM((PEERS, PEERS), i32),
            pltpu.VMEM((TABLES, CAP, PEERS), i32),
            pltpu.VMEM((PEERS, SLOTS, DIM), f32),
            pltpu.VMEM((PEERS, SLOTS, DIM), f32),
            pltpu.VMEM((TABLES, 16, 16, DIM), f32),
            pltpu.VMEM((16, 16, DIM), f32),
            pltpu.VMEM((16, 16, DIM), f32),
            pltpu.VMEM((16, 16, DIM), f32),
            pltpu.VMEM((16, DIM), f32),
            pltpu.VMEM((3, 16, DIM), f32),
            pltpu.VMEM((16, DIM), f32),
            pltpu.VMEM((TABLES, 16, 16, DIM), f32),
            pltpu.SemaphoreType.DMA,
            pltpu.SemaphoreType.DMA((4,)),
            pltpu.SemaphoreType.DMA,
            pltpu.SemaphoreType.DMA,
            pltpu.SemaphoreType.DMA,
            pltpu.SemaphoreType.DMA,
            pltpu.SemaphoreType.DMA,
            pltpu.SemaphoreType.DMA,
            pltpu.SemaphoreType.DMA,
            pltpu.SemaphoreType.DMA,
            pltpu.SemaphoreType.DMA,
            pltpu.SemaphoreType.DMA,
            pltpu.SemaphoreType.DMA((5,)),
            pltpu.SemaphoreType.DMA((5,)),
        ],
        compiler_params=pltpu.CompilerParams(
            collective_id=0, has_side_effects=True, vmem_limit_bytes=48 << 20
        ),
    )(tab, *(pltpu.with_memory_space_constraint(a, HBM) for a in (rows, bags, hot_rows, ids)))
    return out.reshape(BATCH_DEV, TABLES, DIM)


def solution(mesh):
    both = ("gx", "gy")
    return jax.shard_map(
        body,
        mesh=mesh,
        in_specs=(
            P(None, both, None),
            P(both, None, None, None),
            P(both, None, None, None),
            P(),
            P(both, None, None),
        ),
        out_specs=P(both, None, None),
        check_vma=False,
    )
```

```python
import jax
import jax.numpy as jnp
from jax import lax
from jax.experimental import pallas as pl
from jax.experimental.pallas import tpu as pltpu
from jax.sharding import PartitionSpec as P

MESH = pl.DeviceIdType.MESH
HBM = pltpu.MemorySpace.HBM
GX, GY = 8, 16
PEERS = GX * GY
CAP, TABLES, DIM = 16, 2, 128
ROWS_DEV, HOT, HOT_BAG, BATCH_DEV = 8192, 256, 8, 128
SLOTS = TABLES * CAP
GROUP = 32
CUTS = (60, 90)


def hops(offset):
    dz, _, dy, dx = offset
    return sum(min(d, 4 - d) for d in (dz, dy, dx))


def neg(offset):
    dz, dc, dy, dx = offset
    return -dz % 4, dc, -dy % 4, -dx % 4


LINE = [(0, dc, 0, dx) for dx in (1, 3, 2) for dc in (0, 1)]
NEAR = [(0, dc, dy, dx) for dc in (0, 1) for dy in (1, 2, 3) for dx in (1, 2, 3)]
NEAR += [(dz, dc, 0, dx) for dz in (1, 2, 3) for dc in (0, 1) for dx in (1, 2, 3)]

ACROSS = [(u // 8, u // 4 % 2, u % 4, 0) for u in range(1, GROUP)]
BEFORE = [(dz, 0, dy, dx) for dz in (1, 2, 3) for dy in (1, 2, 3) for dx in (1, 3) if (dz + dy) % 2 != dx // 3]


def orders():
    every = [(q // 32, q // 16 % 2, q // 4 % 4, q % 4) for q in (k * STEP % PEERS for k in range(1, PEERS))]
    last = [o for o in every if hops(o) <= LAST]
    corners = [o for o in every if o[0] and o[2] and o[3]]
    planes = [o for o in every if o not in last and o not in corners]
    return planes, corners, last


STEP, LAST = 79, 1


def split_bf16(x):
    high = x.astype(jnp.bfloat16)
    low = (x - high.astype(jnp.float32)).astype(jnp.bfloat16)
    return high, low


def kernel(
    tab_hbm, rows_hbm, bags_hbm, hot_rows_hbm, hot_ids_hbm, out_ref,
    tab, rows_v, bags_v, hot_rows_v, hot_at_v, hot_at, hot_ids_v, msg_t, idx_out, idx_mid, idx_line, idx_near, idx_far, idx_own,
    bags_t, bags_p, lanes, sbuf, rbuf, hot_own, hot_r0, hot_s0, hot_r1, hot_s1, hot_r2, hot_s2, hot_in, hot_pin, hot_ps, hot_all,
    tab_sem, in_sems, at_sem, idx_ssem1, idx_rsem1, idx_ssem2, idx_rsem2, idx_csem, idx_crsem, self_sem,
    row_ssem, row_rsem, h_ssem, h_rsem,
):
    gx, gy = lax.axis_index("gx"), lax.axis_index("gy")
    me = gx * GY + gy
    y, x = gy // 4, lax.rem(gy, 4)
    z, core = gx // 2, lax.rem(gx, 2)

    def at(dz, dc, dy, dx):
        px = lax.rem(z + dz, 4) * 2 + lax.rem(core + dc, 2)
        return px, lax.rem(y + dy, 4) * 4 + lax.rem(x + dx, 4)

    known = [at(*o) for o in sorted(BEFORE + NEAR + ACROSS + LINE, key=hops, reverse=True)]
    beside = [at(b // 4, 0, b % 4, 1 + (b + b // 4) % 2 * 2) for b in range(16)]
    along_x = [at(0, 0, 0, dx) for dx in (1, 2, 3)]

    def unit(px, py):
        return px * 4 + py // 4

    here = unit(gx, gy)
    block = z * 4 + y
    other = 1 - core
    partner = (z * 2 + other, gy)

    def drain(ref, sem):
        pltpu.make_async_copy(ref, ref, sem).wait()

    def hot_send(src, dst, stage, device):
        pltpu.make_async_remote_copy(
            src_ref=src, dst_ref=dst, send_sem=h_ssem.at[stage], recv_sem=h_rsem.at[stage],
            device_id=device, device_id_type=MESH,
        ).start()

    small = [
        pltpu.make_async_copy(rows_hbm, rows_v, in_sems.at[0]),
        pltpu.make_async_copy(hot_rows_hbm, hot_rows_v, in_sems.at[1]),
        pltpu.make_async_copy(bags_hbm, bags_v, in_sems.at[2]),
        pltpu.make_async_copy(hot_ids_hbm, hot_ids_v, in_sems.at[3]),
    ]
    for copy in small:
        copy.start()

    barrier = pltpu.get_barrier_semaphore()
    for device in known:
        pl.semaphore_signal(barrier, inc=1, device_id=device, device_id_type=MESH)
    tab[TABLES * ROWS_DEV] = jnp.zeros((1, DIM), jnp.float32)

    small[0].wait()
    piece = TABLES * ROWS_DEV // 8
    for i in range(8):
        part = pl.ds(i * piece, piece)
        pltpu.make_async_copy(tab_hbm.at[part], tab.at[part], tab_sem).start()
    slot = lax.broadcasted_iota(jnp.int32, (SLOTS, PEERS), 0)
    padded = jnp.concatenate(
        [
            rows_v[...] + jnp.where(slot < CAP, 0, ROWS_DEV),
            jnp.zeros((PEERS - SLOTS, PEERS), jnp.int32),
        ],
        axis=0,
    )
    msg_t[...] = padded.T
    for p in range(PEERS):
        idx_out[p] = msg_t[pl.ds(p, 1), :]
    for d in range(4):
        idx_mid[d, here] = idx_out[here * 4 + d]

    pl.semaphore_wait(barrier, len(known))

    def tell(o, landing, kind):
        px, py = at(*o)
        pltpu.make_async_remote_copy(
            src_ref=idx_out.at[px * GY + py], dst_ref=landing,
            send_sem=idx_csem, recv_sem=idx_crsem.at[kind],
            device_id=(px, py), device_id_type=MESH,
        ).start()

    def tell_group(o):
        px, py = at(*o)
        pltpu.make_async_remote_copy(
            src_ref=idx_out.at[pl.ds(unit(px, py) * 4, 4)], dst_ref=idx_mid.at[:, here],
            send_sem=idx_ssem1, recv_sem=idx_rsem1,
            device_id=(px, py), device_id_type=MESH,
        ).start()

    for o in sorted(NEAR + ACROSS + LINE, key=hops, reverse=True):
        if o in LINE:
            tell(o, idx_line.at[LINE.index(o)], 0)
        elif o in NEAR:
            tell(o, idx_near.at[NEAR.index(o)], 1)
        else:
            tell_group(o)

    small[1].wait()
    local = hot_rows_v[...] - me * ROWS_DEV
    mine = jnp.logical_and(local >= 0, local < ROWS_DEV)
    table = lax.broadcasted_iota(jnp.int32, (TABLES, HOT), 0)
    hot_at_v[...] = jnp.where(mine, local + table * ROWS_DEV, TABLES * ROWS_DEV)
    at_copy = pltpu.make_async_copy(hot_at_v, hot_at, at_sem)
    at_copy.start()
    at_copy.wait()

    drain(tab.at[pl.ds(0, TABLES * ROWS_DEV)], tab_sem)

    for t in range(TABLES):
        for h in range(HOT):
            hot_own[t, h // 16, pl.ds(h % 16, 1), :] = tab[hot_at[t, h]]
    hot_send(hot_own.at[other], hot_r0, 0, partner)

    planes, corners, last = orders()
    sequence = planes + corners + last

    def serve(first, stop):
        for n in range(first, stop):
            o = sequence[n]
            px, py = at(*o)
            u = unit(px, py)
            if o in LINE:
                asked = [idx_line[LINE.index(neg(o)), 0, slot] for slot in range(SLOTS)]
            elif o in NEAR:
                asked = [idx_near[NEAR.index(neg(o)), 0, slot] for slot in range(SLOTS)]
            elif o[3]:
                asked = [idx_far[3 - o[3], u, 0, slot] for slot in range(SLOTS)]
            else:
                asked = [idx_own[u, 0, slot] for slot in range(SLOTS)]
            for slot in range(SLOTS):
                sbuf[n, pl.ds(slot, 1), :] = tab[asked[slot]]
            pltpu.make_async_remote_copy(
                src_ref=sbuf.at[n], dst_ref=rbuf.at[n],
                send_sem=row_ssem, recv_sem=row_rsem.at[n // 16],
                device_id=(px, py), device_id_type=MESH,
            ).start()

    drain(hot_r0, h_rsem.at[0])
    hot_s0[...] = hot_own[core] + hot_r0[...]
    for px, py in beside:
        hot_send(hot_s0.at[px // 2 * 4 + py // 4], hot_r1.at[block], 1, (px, py))

    drain(idx_line, idx_crsem.at[0])
    drain(idx_near, idx_crsem.at[1])

    pltpu.make_async_copy(idx_mid.at[:, pl.ds(0, GROUP - 1)], idx_mid.at[:, pl.ds(0, GROUP - 1)], idx_rsem1).wait()
    for k, device in enumerate(along_x):
        pltpu.make_async_remote_copy(
            src_ref=idx_mid.at[lax.rem(device[1], 4)], dst_ref=idx_far.at[k],
            send_sem=idx_ssem2, recv_sem=idx_rsem2,
            device_id=device, device_id_type=MESH,
        ).start()
    own_idx = pltpu.make_async_copy(idx_mid.at[x], idx_own, self_sem)
    own_idx.start()

    own_idx.wait()

    serve(0, min(CUTS[0], len(planes)))

    drain(hot_r1, h_rsem.at[1])
    total = hot_r1[0]
    for k in range(1, 16):
        total = total + hot_r1[k]
    hot_s1[...] = total
    for k, device in enumerate(along_x):
        hot_send(hot_s1, hot_r2.at[k], 2, device)

    serve(min(CUTS[0], len(planes)), len(planes))

    drain(idx_far, idx_rsem2)

    serve(len(planes), max(CUTS[1], len(planes)))

    drain(hot_r2, h_rsem.at[2])
    total = (hot_s1[...] + hot_r2[0]) + (hot_r2[1] + hot_r2[2])
    hot_s2[...] = total
    for k, device in enumerate(beside[1:]):
        hot_send(hot_s2, hot_in.at[k], 3, device)

    serve(max(CUTS[1], len(planes)), PEERS - 1)

    for slot in range(SLOTS):
        rbuf[PEERS - 1, pl.ds(slot, 1), :] = tab[idx_own[here, 0, slot]]

    small[2].wait()
    bags_t[...] = jnp.concatenate(
        [bags_v[...], jnp.zeros((PEERS - SLOTS, PEERS), jnp.int32)], axis=0
    ).T
    for p in range(PEERS):
        bags_p[p] = bags_t[pl.ds(p, 1), :]
    for n, (dz, dc, dy, dx) in enumerate(sequence + [(0, 0, 0, 0)]):
        px, py = at(*neg((dz, dc, dy, dx)))
        bags_t[pl.ds(n, 1), :] = bags_p[px * GY + py]
    lane = lax.broadcasted_iota(jnp.int32, (CAP, PEERS), 1)
    for t in range(TABLES):
        line = jnp.zeros((CAP, PEERS), jnp.int32)
        for j in range(8):
            part = bags_t[pl.ds(j, 16, stride=8), :]
            moved = pltpu.roll(part, (j * CAP - t * CAP) % PEERS, axis=1)
            line = jnp.where(lane // CAP == j, moved, line)
        lanes[t] = line

    small[3].wait()
    drain(hot_in, h_rsem.at[3])
    hot_send(hot_in, hot_pin, 4, partner)
    hot_send(hot_s2, hot_ps, 5, partner)

    drain(hot_pin, h_rsem.at[4])
    drain(hot_ps, h_rsem.at[5])
    hot_all[core, block] = hot_s2[...]
    hot_all[other, block] = hot_ps[...]
    for b in range(1, 16):
        from_b = lax.rem(z + 4 - b // 4, 4) * 4 + lax.rem(y + 4 - b % 4, 4)
        hot_all[core, from_b] = hot_in[b - 1]
        hot_all[other, from_b] = hot_pin[b - 1]
    spot = lax.broadcasted_iota(jnp.int32, (HOT, BATCH_DEV), 0)
    sample = lax.broadcasted_iota(jnp.int32, (BATCH_DEV, 2 * PEERS), 0)
    parts = []
    for t in range(TABLES):
        counts = jnp.zeros((HOT, BATCH_DEV), jnp.float32)
        for k in range(HOT_BAG):
            ids = hot_ids_v[pl.ds(t * HOT_BAG + k, 1), :]
            counts = counts + jnp.where(ids == spot, 1.0, 0.0)
        counts = counts.T.astype(jnp.bfloat16)
        high, low = split_bf16(hot_all[t].reshape(HOT, DIM))
        both = jnp.concatenate([high, low], axis=1)
        parts.append(jnp.dot(counts, both, preferred_element_type=jnp.float32))

    for q in range(8):
        drain(rbuf.at[pl.ds(q * 16, 16 if q < 7 else 15)], row_rsem.at[q])
        for t in range(TABLES):
            wanted = jnp.concatenate(
                [lanes[t, pl.ds(2 * q, 1), :], lanes[t, pl.ds(2 * q + 1, 1), :]], axis=1
            )
            onehot = jnp.where(wanted == sample, 1.0, 0.0).astype(jnp.bfloat16)
            rows = rbuf[pl.ds(q * 16, 16), pl.ds(t * CAP, CAP), :].reshape(256, DIM)
            high, low = split_bf16(rows)
            both = jnp.concatenate([high, low], axis=1)
            parts[t] = parts[t] + jnp.dot(onehot, both, preferred_element_type=jnp.float32)
    for t in range(TABLES):
        out_ref[pl.ds(t, BATCH_DEV, stride=2), :] = parts[t][:, :DIM] + parts[t][:, DIM:]

    drain(idx_out.at[pl.ds(0, 4 * (GROUP - 1))], idx_ssem1)
    drain(idx_far, idx_ssem2)
    drain(idx_out.at[pl.ds(0, len(LINE + NEAR))], idx_csem)
    drain(sbuf.at[pl.ds(0, PEERS - 1)], row_ssem)
    for stage, ref in enumerate((hot_r0, hot_r1, hot_r2, hot_in, hot_pin, hot_ps)):
        drain(ref, h_ssem.at[stage])


def body(tables, cold_rows, cold_bags, hot_rows, hot_ids):
    tab = tables.reshape(TABLES * ROWS_DEV, 1, DIM)
    rows = cold_rows[0].transpose(0, 2, 1).reshape(SLOTS, PEERS)
    bags = cold_bags[0].transpose(0, 2, 1).reshape(SLOTS, PEERS)
    ids = hot_ids.transpose(1, 2, 0).reshape(TABLES * HOT_BAG, BATCH_DEV)
    f32, i32 = jnp.float32, jnp.int32
    out = pl.pallas_call(
        kernel,
        out_shape=jax.ShapeDtypeStruct((BATCH_DEV * TABLES, DIM), f32),
        in_specs=[pl.BlockSpec(memory_space=HBM)] * 5,
        out_specs=pl.BlockSpec(memory_space=pltpu.VMEM),
        scratch_shapes=[
            pltpu.VMEM((TABLES * ROWS_DEV + 1, 1, DIM), f32),
            pltpu.VMEM((SLOTS, PEERS), i32),
            pltpu.VMEM((SLOTS, PEERS), i32),
            pltpu.VMEM((TABLES, HOT), i32),
            pltpu.VMEM((TABLES, HOT), i32),
            pltpu.SMEM((TABLES, HOT), i32),
            pltpu.VMEM((TABLES * HOT_BAG, BATCH_DEV), i32),
            pltpu.VMEM((PEERS, PEERS), i32),
            pltpu.VMEM((PEERS, 1, PEERS), i32),
            pltpu.VMEM((4, GROUP, 1, PEERS), i32),
            pltpu.SMEM((len(LINE), 1, PEERS), i32),
            pltpu.SMEM((len(NEAR), 1, PEERS), i32),
            pltpu.SMEM((3, GROUP, 1, PEERS), i32),
            pltpu.SMEM((GROUP, 1, PEERS), i32),
            pltpu.VMEM((PEERS, PEERS), i32),
            pltpu.VMEM((PEERS, 1, PEERS), i32),
            pltpu.VMEM((TABLES, CAP, PEERS), i32),
            pltpu.VMEM((PEERS, SLOTS, DIM), f32),
            pltpu.VMEM((PEERS, SLOTS, DIM), f32),
            pltpu.VMEM((TABLES, 16, 16, DIM), f32),
            pltpu.VMEM((16, 16, DIM), f32),
            pltpu.VMEM((16, 16, DIM), f32),
            pltpu.VMEM((16, 16, DIM), f32),
            pltpu.VMEM((16, DIM), f32),
            pltpu.VMEM((3, 16, DIM), f32),
            pltpu.VMEM((16, DIM), f32),
            pltpu.VMEM((15, 16, DIM), f32),
            pltpu.VMEM((15, 16, DIM), f32),
            pltpu.VMEM((16, DIM), f32),
            pltpu.VMEM((TABLES, 16, 16, DIM), f32),
            pltpu.SemaphoreType.DMA,
            pltpu.SemaphoreType.DMA((4,)),
            pltpu.SemaphoreType.DMA,
            pltpu.SemaphoreType.DMA,
            pltpu.SemaphoreType.DMA,
            pltpu.SemaphoreType.DMA,
            pltpu.SemaphoreType.DMA,
            pltpu.SemaphoreType.DMA,
            pltpu.SemaphoreType.DMA((2,)),
            pltpu.SemaphoreType.DMA,
            pltpu.SemaphoreType.DMA,
            pltpu.SemaphoreType.DMA((8,)),
            pltpu.SemaphoreType.DMA((6,)),
            pltpu.SemaphoreType.DMA((6,)),
        ],
        compiler_params=pltpu.CompilerParams(
            collective_id=0, has_side_effects=True, vmem_limit_bytes=48 << 20
        ),
    )(tab, *(pltpu.with_memory_space_constraint(a, HBM) for a in (rows, bags, hot_rows, ids)))
    return out.reshape(BATCH_DEV, TABLES, DIM)


def solution(mesh):
    both = ("gx", "gy")
    return jax.shard_map(
        body,
        mesh=mesh,
        in_specs=(
            P(None, both, None),
            P(both, None, None, None),
            P(both, None, None, None),
            P(),
            P(both, None, None),
        ),
        out_specs=P(both, None, None),
        check_vma=False,
    )
```

```python
import jax
import jax.numpy as jnp
from jax import lax
from jax.experimental import pallas as pl
from jax.experimental.pallas import tpu as pltpu
from jax.sharding import PartitionSpec as P

MESH = pl.DeviceIdType.MESH
HBM = pltpu.MemorySpace.HBM
GX, GY = 8, 16
PEERS = GX * GY
CAP, TABLES, DIM = 16, 2, 128
ROWS_DEV, HOT, HOT_BAG, BATCH_DEV = 8192, 256, 8, 128
SLOTS = TABLES * CAP
GROUP = 32
CUTS = (30, 85)


def hops(offset):
    dz, _, dy, dx = offset
    return sum(min(d, 4 - d) for d in (dz, dy, dx))


def neg(offset):
    dz, dc, dy, dx = offset
    return -dz % 4, dc, -dy % 4, -dx % 4


LINE = [(0, dc, 0, dx) for dx in (1, 3, 2) for dc in (0, 1)]
NEAR = [(0, dc, dy, dx) for dc in (0, 1) for dy in (1, 2, 3) for dx in (1, 2, 3)]
NEAR += [(dz, dc, 0, dx) for dz in (1, 2, 3) for dc in (0, 1) for dx in (1, 2, 3)]

ACROSS = [(u // 8, u // 4 % 2, u % 4, 0) for u in range(1, GROUP)]
BEFORE = [(dz, 0, dy, dx) for dz in (1, 2, 3) for dy in (1, 2, 3) for dx in (1, 3) if (dz + dy) % 2 != dx // 3]


def orders():
    every = [(q // 32, q // 16 % 2, q // 4 % 4, q % 4) for q in (k * STEP % PEERS for k in range(1, PEERS))]
    last = [o for o in every if hops(o) <= LAST]
    corners = [o for o in every if o[0] and o[2] and o[3]]
    planes = [o for o in every if o not in last and o not in corners]
    return planes, corners, last


STEP, LAST = 79, 1


def split_bf16(x):
    high = x.astype(jnp.bfloat16)
    low = (x - high.astype(jnp.float32)).astype(jnp.bfloat16)
    return high, low


def kernel(
    tab_hbm, rows_hbm, bags_hbm, hot_rows_hbm, hot_ids_hbm, out_ref,
    tab, rows_v, bags_v, hot_rows_v, hot_at_v, hot_at, hot_ids_v, msg_t, idx_out, idx_mid, idx_line, idx_near, idx_far, idx_own,
    bags_t, bags_p, lanes, sbuf, rbuf, hot_own, hot_r0, hot_s0, hot_r1, hot_s1, hot_r2, hot_s2, hot_in, hot_pin, hot_ps, hot_all,
    tab_sem, in_sems, at_sem, idx_ssem1, idx_rsem1, idx_ssem2, idx_rsem2, idx_csem, idx_crsem, self_sem,
    row_ssem, row_rsem, h_ssem, h_rsem,
):
    gx, gy = lax.axis_index("gx"), lax.axis_index("gy")
    me = gx * GY + gy
    y, x = gy // 4, lax.rem(gy, 4)
    z, core = gx // 2, lax.rem(gx, 2)

    def at(dz, dc, dy, dx):
        px = lax.rem(z + dz, 4) * 2 + lax.rem(core + dc, 2)
        return px, lax.rem(y + dy, 4) * 4 + lax.rem(x + dx, 4)

    known = [at(*o) for o in sorted(BEFORE + NEAR + ACROSS + LINE, key=hops, reverse=True)]
    beside = [at(b // 4, 0, b % 4, 1 + (b + b // 4) % 2 * 2) for b in range(16)]
    along_x = [at(0, 0, 0, dx) for dx in (1, 2, 3)]

    def unit(px, py):
        return px * 4 + py // 4

    here = unit(gx, gy)
    block = z * 4 + y
    other = 1 - core
    partner = (z * 2 + other, gy)

    def drain(ref, sem):
        pltpu.make_async_copy(ref, ref, sem).wait()

    def hot_send(src, dst, stage, device):
        pltpu.make_async_remote_copy(
            src_ref=src, dst_ref=dst, send_sem=h_ssem.at[stage], recv_sem=h_rsem.at[stage],
            device_id=device, device_id_type=MESH,
        ).start()

    small = [
        pltpu.make_async_copy(rows_hbm, rows_v, in_sems.at[0]),
        pltpu.make_async_copy(hot_rows_hbm, hot_rows_v, in_sems.at[1]),
        pltpu.make_async_copy(bags_hbm, bags_v, in_sems.at[2]),
        pltpu.make_async_copy(hot_ids_hbm, hot_ids_v, in_sems.at[3]),
    ]
    for copy in small:
        copy.start()

    barrier = pltpu.get_barrier_semaphore()
    for device in known:
        pl.semaphore_signal(barrier, inc=1, device_id=device, device_id_type=MESH)
    tab[TABLES * ROWS_DEV] = jnp.zeros((1, DIM), jnp.float32)

    small[0].wait()
    piece = TABLES * ROWS_DEV // 8
    for i in range(8):
        part = pl.ds(i * piece, piece)
        pltpu.make_async_copy(tab_hbm.at[part], tab.at[part], tab_sem).start()
    slot = lax.broadcasted_iota(jnp.int32, (SLOTS, PEERS), 0)
    padded = jnp.concatenate(
        [
            rows_v[...] + jnp.where(slot < CAP, 0, ROWS_DEV),
            jnp.zeros((PEERS - SLOTS, PEERS), jnp.int32),
        ],
        axis=0,
    )
    msg_t[...] = padded.T
    for p in range(PEERS):
        idx_out[p] = msg_t[pl.ds(p, 1), :]
    for d in range(4):
        idx_mid[d, here] = idx_out[here * 4 + d]

    pl.semaphore_wait(barrier, len(known))

    def tell(o, landing, kind):
        px, py = at(*o)
        pltpu.make_async_remote_copy(
            src_ref=idx_out.at[px * GY + py], dst_ref=landing,
            send_sem=idx_csem, recv_sem=idx_crsem.at[kind],
            device_id=(px, py), device_id_type=MESH,
        ).start()

    def tell_group(o):
        px, py = at(*o)
        pltpu.make_async_remote_copy(
            src_ref=idx_out.at[pl.ds(unit(px, py) * 4, 4)], dst_ref=idx_mid.at[:, here],
            send_sem=idx_ssem1, recv_sem=idx_rsem1,
            device_id=(px, py), device_id_type=MESH,
        ).start()

    for o in sorted(NEAR + ACROSS + LINE, key=hops, reverse=True):
        if o in LINE:
            tell(o, idx_line.at[LINE.index(o)], 0)
        elif o in NEAR:
            tell(o, idx_near.at[NEAR.index(o)], 1)
        else:
            tell_group(o)

    small[1].wait()
    local = hot_rows_v[...] - me * ROWS_DEV
    mine = jnp.logical_and(local >= 0, local < ROWS_DEV)
    table = lax.broadcasted_iota(jnp.int32, (TABLES, HOT), 0)
    hot_at_v[...] = jnp.where(mine, local + table * ROWS_DEV, TABLES * ROWS_DEV)
    at_copy = pltpu.make_async_copy(hot_at_v, hot_at, at_sem)
    at_copy.start()
    at_copy.wait()

    drain(tab.at[pl.ds(0, TABLES * ROWS_DEV)], tab_sem)

    for t in range(TABLES):
        for h in range(HOT):
            hot_own[t, h // 16, pl.ds(h % 16, 1), :] = tab[hot_at[t, h]]
    hot_send(hot_own.at[other], hot_r0, 0, partner)

    planes, corners, last = orders()
    sequence = planes + corners + last

    def serve(first, stop):
        ready = []
        for n in range(first, stop):
            o = sequence[n]
            px, py = at(*o)
            u = unit(px, py)
            if o in LINE:
                asked = [idx_line[LINE.index(neg(o)), 0, slot] for slot in range(SLOTS)]
            elif o in NEAR:
                asked = [idx_near[NEAR.index(neg(o)), 0, slot] for slot in range(SLOTS)]
            elif o[3]:
                asked = [idx_far[3 - o[3], u, 0, slot] for slot in range(SLOTS)]
            else:
                asked = [idx_own[u, 0, slot] for slot in range(SLOTS)]
            for slot in range(SLOTS):
                sbuf[n, pl.ds(slot, 1), :] = tab[asked[slot]]
            copy = pltpu.make_async_remote_copy(
                src_ref=sbuf.at[n], dst_ref=rbuf.at[n],
                send_sem=row_ssem, recv_sem=row_rsem.at[n // 16],
                device_id=(px, py), device_id_type=MESH,
            )
            ready.append(copy)
            if len(ready) > 1:
                ready.pop(0).start()
        for copy in ready:
            copy.start()

    drain(hot_r0, h_rsem.at[0])
    hot_s0[...] = hot_own[core] + hot_r0[...]
    for px, py in beside:
        hot_send(hot_s0.at[px // 2 * 4 + py // 4], hot_r1.at[block], 1, (px, py))

    drain(idx_line, idx_crsem.at[0])
    drain(idx_near, idx_crsem.at[1])

    pltpu.make_async_copy(idx_mid.at[:, pl.ds(0, GROUP - 1)], idx_mid.at[:, pl.ds(0, GROUP - 1)], idx_rsem1).wait()
    for k, device in enumerate(along_x):
        pltpu.make_async_remote_copy(
            src_ref=idx_mid.at[lax.rem(device[1], 4)], dst_ref=idx_far.at[k],
            send_sem=idx_ssem2, recv_sem=idx_rsem2,
            device_id=device, device_id_type=MESH,
        ).start()
    own_idx = pltpu.make_async_copy(idx_mid.at[x], idx_own, self_sem)
    own_idx.start()

    own_idx.wait()

    serve(0, min(CUTS[0], len(planes)))

    drain(hot_r1, h_rsem.at[1])
    total = hot_r1[0]
    for k in range(1, 16):
        total = total + hot_r1[k]
    hot_s1[...] = total
    for k, device in enumerate(along_x):
        hot_send(hot_s1, hot_r2.at[k], 2, device)

    serve(min(CUTS[0], len(planes)), len(planes))

    drain(idx_far, idx_rsem2)

    serve(len(planes), max(CUTS[1], len(planes)))

    drain(hot_r2, h_rsem.at[2])
    total = (hot_s1[...] + hot_r2[0]) + (hot_r2[1] + hot_r2[2])
    hot_s2[...] = total
    for k, device in enumerate(beside[1:]):
        hot_send(hot_s2, hot_in.at[k], 3, device)

    serve(max(CUTS[1], len(planes)), PEERS - 1)

    for slot in range(SLOTS):
        rbuf[PEERS - 1, pl.ds(slot, 1), :] = tab[idx_own[here, 0, slot]]

    small[2].wait()
    bags_t[...] = jnp.concatenate(
        [bags_v[...], jnp.zeros((PEERS - SLOTS, PEERS), jnp.int32)], axis=0
    ).T
    for p in range(PEERS):
        bags_p[p] = bags_t[pl.ds(p, 1), :]
    for n, (dz, dc, dy, dx) in enumerate(sequence + [(0, 0, 0, 0)]):
        px, py = at(*neg((dz, dc, dy, dx)))
        bags_t[pl.ds(n, 1), :] = bags_p[px * GY + py]
    lane = lax.broadcasted_iota(jnp.int32, (CAP, PEERS), 1)
    for t in range(TABLES):
        line = jnp.zeros((CAP, PEERS), jnp.int32)
        for j in range(8):
            part = bags_t[pl.ds(j, 16, stride=8), :]
            moved = pltpu.roll(part, (j * CAP - t * CAP) % PEERS, axis=1)
            line = jnp.where(lane // CAP == j, moved, line)
        lanes[t] = line

    small[3].wait()
    drain(hot_in, h_rsem.at[3])
    hot_send(hot_in, hot_pin, 4, partner)
    hot_send(hot_s2, hot_ps, 5, partner)

    drain(hot_pin, h_rsem.at[4])
    drain(hot_ps, h_rsem.at[5])
    hot_all[core, block] = hot_s2[...]
    hot_all[other, block] = hot_ps[...]
    for b in range(1, 16):
        from_b = lax.rem(z + 4 - b // 4, 4) * 4 + lax.rem(y + 4 - b % 4, 4)
        hot_all[core, from_b] = hot_in[b - 1]
        hot_all[other, from_b] = hot_pin[b - 1]
    spot = lax.broadcasted_iota(jnp.int32, (HOT, BATCH_DEV), 0)
    sample = lax.broadcasted_iota(jnp.int32, (BATCH_DEV, 2 * PEERS), 0)
    parts = []
    for t in range(TABLES):
        counts = jnp.zeros((HOT, BATCH_DEV), jnp.float32)
        for k in range(HOT_BAG):
            ids = hot_ids_v[pl.ds(t * HOT_BAG + k, 1), :]
            counts = counts + jnp.where(ids == spot, 1.0, 0.0)
        counts = counts.T.astype(jnp.bfloat16)
        high, low = split_bf16(hot_all[t].reshape(HOT, DIM))
        both = jnp.concatenate([high, low], axis=1)
        parts.append(jnp.dot(counts, both, preferred_element_type=jnp.float32))

    for q in range(8):
        drain(rbuf.at[pl.ds(q * 16, 16 if q < 7 else 15)], row_rsem.at[q])
        for t in range(TABLES):
            wanted = jnp.concatenate(
                [lanes[t, pl.ds(2 * q, 1), :], lanes[t, pl.ds(2 * q + 1, 1), :]], axis=1
            )
            onehot = jnp.where(wanted == sample, 1.0, 0.0).astype(jnp.bfloat16)
            rows = rbuf[pl.ds(q * 16, 16), pl.ds(t * CAP, CAP), :].reshape(256, DIM)
            high, low = split_bf16(rows)
            both = jnp.concatenate([high, low], axis=1)
            parts[t] = parts[t] + jnp.dot(onehot, both, preferred_element_type=jnp.float32)
    for t in range(TABLES):
        out_ref[pl.ds(t, BATCH_DEV, stride=2), :] = parts[t][:, :DIM] + parts[t][:, DIM:]

    drain(idx_out.at[pl.ds(0, 4 * (GROUP - 1))], idx_ssem1)
    drain(idx_far, idx_ssem2)
    drain(idx_out.at[pl.ds(0, len(LINE + NEAR))], idx_csem)
    drain(sbuf.at[pl.ds(0, PEERS - 1)], row_ssem)
    for stage, ref in enumerate((hot_r0, hot_r1, hot_r2, hot_in, hot_pin, hot_ps)):
        drain(ref, h_ssem.at[stage])


def body(tables, cold_rows, cold_bags, hot_rows, hot_ids):
    tab = tables.reshape(TABLES * ROWS_DEV, 1, DIM)
    rows = cold_rows[0].transpose(0, 2, 1).reshape(SLOTS, PEERS)
    bags = cold_bags[0].transpose(0, 2, 1).reshape(SLOTS, PEERS)
    ids = hot_ids.transpose(1, 2, 0).reshape(TABLES * HOT_BAG, BATCH_DEV)
    f32, i32 = jnp.float32, jnp.int32
    out = pl.pallas_call(
        kernel,
        out_shape=jax.ShapeDtypeStruct((BATCH_DEV * TABLES, DIM), f32),
        in_specs=[pl.BlockSpec(memory_space=HBM)] * 5,
        out_specs=pl.BlockSpec(memory_space=pltpu.VMEM),
        scratch_shapes=[
            pltpu.VMEM((TABLES * ROWS_DEV + 1, 1, DIM), f32),
            pltpu.VMEM((SLOTS, PEERS), i32),
            pltpu.VMEM((SLOTS, PEERS), i32),
            pltpu.VMEM((TABLES, HOT), i32),
            pltpu.VMEM((TABLES, HOT), i32),
            pltpu.SMEM((TABLES, HOT), i32),
            pltpu.VMEM((TABLES * HOT_BAG, BATCH_DEV), i32),
            pltpu.VMEM((PEERS, PEERS), i32),
            pltpu.VMEM((PEERS, 1, PEERS), i32),
            pltpu.VMEM((4, GROUP, 1, PEERS), i32),
            pltpu.SMEM((len(LINE), 1, PEERS), i32),
            pltpu.SMEM((len(NEAR), 1, PEERS), i32),
            pltpu.SMEM((3, GROUP, 1, PEERS), i32),
            pltpu.SMEM((GROUP, 1, PEERS), i32),
            pltpu.VMEM((PEERS, PEERS), i32),
            pltpu.VMEM((PEERS, 1, PEERS), i32),
            pltpu.VMEM((TABLES, CAP, PEERS), i32),
            pltpu.VMEM((PEERS, SLOTS, DIM), f32),
            pltpu.VMEM((PEERS, SLOTS, DIM), f32),
            pltpu.VMEM((TABLES, 16, 16, DIM), f32),
            pltpu.VMEM((16, 16, DIM), f32),
            pltpu.VMEM((16, 16, DIM), f32),
            pltpu.VMEM((16, 16, DIM), f32),
            pltpu.VMEM((16, DIM), f32),
            pltpu.VMEM((3, 16, DIM), f32),
            pltpu.VMEM((16, DIM), f32),
            pltpu.VMEM((15, 16, DIM), f32),
            pltpu.VMEM((15, 16, DIM), f32),
            pltpu.VMEM((16, DIM), f32),
            pltpu.VMEM((TABLES, 16, 16, DIM), f32),
            pltpu.SemaphoreType.DMA,
            pltpu.SemaphoreType.DMA((4,)),
            pltpu.SemaphoreType.DMA,
            pltpu.SemaphoreType.DMA,
            pltpu.SemaphoreType.DMA,
            pltpu.SemaphoreType.DMA,
            pltpu.SemaphoreType.DMA,
            pltpu.SemaphoreType.DMA,
            pltpu.SemaphoreType.DMA((2,)),
            pltpu.SemaphoreType.DMA,
            pltpu.SemaphoreType.DMA,
            pltpu.SemaphoreType.DMA((8,)),
            pltpu.SemaphoreType.DMA((6,)),
            pltpu.SemaphoreType.DMA((6,)),
        ],
        compiler_params=pltpu.CompilerParams(
            collective_id=0, has_side_effects=True, vmem_limit_bytes=48 << 20
        ),
    )(tab, *(pltpu.with_memory_space_constraint(a, HBM) for a in (rows, bags, hot_rows, ids)))
    return out.reshape(BATCH_DEV, TABLES, DIM)


def solution(mesh):
    both = ("gx", "gy")
    return jax.shard_map(
        body,
        mesh=mesh,
        in_specs=(
            P(None, both, None),
            P(both, None, None, None),
            P(both, None, None, None),
            P(),
            P(both, None, None),
        ),
        out_specs=P(both, None, None),
        check_vma=False,
    )
```

```python
import jax
import jax.numpy as jnp
from jax import lax
from jax.experimental import pallas as pl
from jax.experimental.pallas import tpu as pltpu
from jax.sharding import PartitionSpec as P

MESH = pl.DeviceIdType.MESH
HBM = pltpu.MemorySpace.HBM
GX, GY = 8, 16
PEERS = GX * GY
CAP, TABLES, DIM = 16, 2, 128
ROWS_DEV, HOT, HOT_BAG, BATCH_DEV = 8192, 256, 8, 128
SLOTS = TABLES * CAP
GROUP = 32
CUTS = (30, 85)
HEAD = 16


def hops(offset):
    dz, _, dy, dx = offset
    return sum(min(d, 4 - d) for d in (dz, dy, dx))


def neg(offset):
    dz, dc, dy, dx = offset
    return -dz % 4, dc, -dy % 4, -dx % 4


LINE = [(0, dc, 0, dx) for dx in (1, 3, 2) for dc in (0, 1)]
NEAR = [(0, dc, dy, dx) for dc in (0, 1) for dy in (1, 2, 3) for dx in (1, 2, 3)]
NEAR += [(dz, dc, 0, dx) for dz in (1, 2, 3) for dc in (0, 1) for dx in (1, 2, 3)]

ACROSS = [(u // 8, u // 4 % 2, u % 4, 0) for u in range(1, GROUP)]
BEFORE = [(dz, 0, dy, dx) for dz in (1, 2, 3) for dy in (1, 2, 3) for dx in (1, 3) if (dz + dy) % 2 != dx // 3]


def orders():
    every = [(q // 32, q // 16 % 2, q // 4 % 4, q % 4) for q in (k * STEP % PEERS for k in range(1, PEERS))]
    last = [o for o in every if hops(o) <= LAST]
    corners = [o for o in every if o[0] and o[2] and o[3]]
    planes = [o for o in every if o not in last and o not in corners]
    head = [o for o in planes if o[3]][:HEAD]
    planes = head + [o for o in planes if o not in head]
    return planes, corners, last


STEP, LAST = 79, 1


def split_bf16(x):
    high = x.astype(jnp.bfloat16)
    low = (x - high.astype(jnp.float32)).astype(jnp.bfloat16)
    return high, low


def kernel(
    tab_hbm, rows_hbm, bags_hbm, hot_rows_hbm, hot_ids_hbm, out_ref,
    tab, rows_v, bags_v, hot_rows_v, hot_at_v, hot_at, hot_ids_v, msg_t, idx_out, idx_mid, idx_line, idx_near, idx_far, idx_own,
    bags_t, bags_p, lanes, sbuf, rbuf, hot_own, hot_r0, hot_s0, hot_r1, hot_s1, hot_r2, hot_s2, hot_in, hot_pin, hot_ps, hot_all,
    tab_sem, in_sems, at_sem, idx_ssem1, idx_rsem1, idx_ssem2, idx_rsem2, idx_csem, idx_crsem, self_sem,
    row_ssem, row_rsem, h_ssem, h_rsem,
):
    gx, gy = lax.axis_index("gx"), lax.axis_index("gy")
    me = gx * GY + gy
    y, x = gy // 4, lax.rem(gy, 4)
    z, core = gx // 2, lax.rem(gx, 2)

    def at(dz, dc, dy, dx):
        px = lax.rem(z + dz, 4) * 2 + lax.rem(core + dc, 2)
        return px, lax.rem(y + dy, 4) * 4 + lax.rem(x + dx, 4)

    known = [at(*o) for o in sorted(BEFORE + NEAR + ACROSS + LINE, key=hops, reverse=True)]
    beside = [at(b // 4, 0, b % 4, 1 + (b + b // 4) % 2 * 2) for b in range(16)]
    along_x = [at(0, 0, 0, dx) for dx in (1, 2, 3)]

    def unit(px, py):
        return px * 4 + py // 4

    here = unit(gx, gy)
    block = z * 4 + y
    other = 1 - core
    partner = (z * 2 + other, gy)

    def drain(ref, sem):
        pltpu.make_async_copy(ref, ref, sem).wait()

    def hot_send(src, dst, stage, device):
        pltpu.make_async_remote_copy(
            src_ref=src, dst_ref=dst, send_sem=h_ssem.at[stage], recv_sem=h_rsem.at[stage],
            device_id=device, device_id_type=MESH,
        ).start()

    small = [
        pltpu.make_async_copy(rows_hbm, rows_v, in_sems.at[0]),
        pltpu.make_async_copy(hot_rows_hbm, hot_rows_v, in_sems.at[1]),
        pltpu.make_async_copy(bags_hbm, bags_v, in_sems.at[2]),
        pltpu.make_async_copy(hot_ids_hbm, hot_ids_v, in_sems.at[3]),
    ]
    for copy in small:
        copy.start()

    barrier = pltpu.get_barrier_semaphore()
    for device in known:
        pl.semaphore_signal(barrier, inc=1, device_id=device, device_id_type=MESH)
    tab[TABLES * ROWS_DEV] = jnp.zeros((1, DIM), jnp.float32)

    small[0].wait()
    piece = TABLES * ROWS_DEV // 8
    for i in range(8):
        part = pl.ds(i * piece, piece)
        pltpu.make_async_copy(tab_hbm.at[part], tab.at[part], tab_sem).start()
    slot = lax.broadcasted_iota(jnp.int32, (SLOTS, PEERS), 0)
    padded = jnp.concatenate(
        [
            rows_v[...] + jnp.where(slot < CAP, 0, ROWS_DEV),
            jnp.zeros((PEERS - SLOTS, PEERS), jnp.int32),
        ],
        axis=0,
    )
    msg_t[...] = padded.T
    for p in range(PEERS):
        idx_out[p] = msg_t[pl.ds(p, 1), :]
    for d in range(4):
        idx_mid[d, here] = idx_out[here * 4 + d]

    pl.semaphore_wait(barrier, len(known))

    def tell(o, landing, kind):
        px, py = at(*o)
        pltpu.make_async_remote_copy(
            src_ref=idx_out.at[px * GY + py], dst_ref=landing,
            send_sem=idx_csem, recv_sem=idx_crsem.at[kind],
            device_id=(px, py), device_id_type=MESH,
        ).start()

    def tell_group(o):
        px, py = at(*o)
        pltpu.make_async_remote_copy(
            src_ref=idx_out.at[pl.ds(unit(px, py) * 4, 4)], dst_ref=idx_mid.at[:, here],
            send_sem=idx_ssem1, recv_sem=idx_rsem1,
            device_id=(px, py), device_id_type=MESH,
        ).start()

    for o in sorted(NEAR + ACROSS + LINE, key=hops, reverse=True):
        if o in LINE:
            tell(o, idx_line.at[LINE.index(o)], 0)
        elif o in NEAR:
            tell(o, idx_near.at[NEAR.index(o)], 1)
        else:
            tell_group(o)

    small[1].wait()
    local = hot_rows_v[...] - me * ROWS_DEV
    mine = jnp.logical_and(local >= 0, local < ROWS_DEV)
    table = lax.broadcasted_iota(jnp.int32, (TABLES, HOT), 0)
    hot_at_v[...] = jnp.where(mine, local + table * ROWS_DEV, TABLES * ROWS_DEV)
    at_copy = pltpu.make_async_copy(hot_at_v, hot_at, at_sem)
    at_copy.start()
    at_copy.wait()

    drain(tab.at[pl.ds(0, TABLES * ROWS_DEV)], tab_sem)

    for t in range(TABLES):
        for h in range(HOT):
            hot_own[t, h // 16, pl.ds(h % 16, 1), :] = tab[hot_at[t, h]]
    hot_send(hot_own.at[other], hot_r0, 0, partner)

    planes, corners, last = orders()
    sequence = planes + corners + last

    def serve(first, stop):
        ready = []
        for n in range(first, stop):
            o = sequence[n]
            px, py = at(*o)
            u = unit(px, py)
            if o in LINE:
                asked = [idx_line[LINE.index(neg(o)), 0, slot] for slot in range(SLOTS)]
            elif o in NEAR:
                asked = [idx_near[NEAR.index(neg(o)), 0, slot] for slot in range(SLOTS)]
            elif o[3]:
                asked = [idx_far[3 - o[3], u, 0, slot] for slot in range(SLOTS)]
            else:
                asked = [idx_own[u, 0, slot] for slot in range(SLOTS)]
            for slot in range(SLOTS):
                sbuf[n, pl.ds(slot, 1), :] = tab[asked[slot]]
            copy = pltpu.make_async_remote_copy(
                src_ref=sbuf.at[n], dst_ref=rbuf.at[n],
                send_sem=row_ssem, recv_sem=row_rsem.at[n // 16],
                device_id=(px, py), device_id_type=MESH,
            )
            ready.append(copy)
            if len(ready) > 1:
                ready.pop(0).start()
        for copy in ready:
            copy.start()

    drain(hot_r0, h_rsem.at[0])
    hot_s0[...] = hot_own[core] + hot_r0[...]
    for px, py in beside:
        hot_send(hot_s0.at[px // 2 * 4 + py // 4], hot_r1.at[block], 1, (px, py))

    drain(idx_line, idx_crsem.at[0])
    drain(idx_near, idx_crsem.at[1])

    pltpu.make_async_copy(idx_mid.at[:, pl.ds(0, GROUP - 1)], idx_mid.at[:, pl.ds(0, GROUP - 1)], idx_rsem1).wait()
    for k, device in enumerate(along_x):
        pltpu.make_async_remote_copy(
            src_ref=idx_mid.at[lax.rem(device[1], 4)], dst_ref=idx_far.at[k],
            send_sem=idx_ssem2, recv_sem=idx_rsem2,
            device_id=device, device_id_type=MESH,
        ).start()
    own_idx = pltpu.make_async_copy(idx_mid.at[x], idx_own, self_sem)
    own_idx.start()

    serve(0, HEAD)
    own_idx.wait()

    serve(HEAD, min(CUTS[0], len(planes)))

    drain(hot_r1, h_rsem.at[1])
    total = hot_r1[0]
    for k in range(1, 16):
        total = total + hot_r1[k]
    hot_s1[...] = total
    for k, device in enumerate(along_x):
        hot_send(hot_s1, hot_r2.at[k], 2, device)

    serve(min(CUTS[0], len(planes)), len(planes))

    drain(idx_far, idx_rsem2)

    serve(len(planes), max(CUTS[1], len(planes)))

    drain(hot_r2, h_rsem.at[2])
    total = (hot_s1[...] + hot_r2[0]) + (hot_r2[1] + hot_r2[2])
    hot_s2[...] = total
    for k, device in enumerate(beside[1:]):
        hot_send(hot_s2, hot_in.at[k], 3, device)

    serve(max(CUTS[1], len(planes)), PEERS - 1)

    for slot in range(SLOTS):
        rbuf[PEERS - 1, pl.ds(slot, 1), :] = tab[idx_own[here, 0, slot]]

    small[2].wait()
    bags_t[...] = jnp.concatenate(
        [bags_v[...], jnp.zeros((PEERS - SLOTS, PEERS), jnp.int32)], axis=0
    ).T
    for p in range(PEERS):
        bags_p[p] = bags_t[pl.ds(p, 1), :]
    for n, (dz, dc, dy, dx) in enumerate(sequence + [(0, 0, 0, 0)]):
        px, py = at(*neg((dz, dc, dy, dx)))
        bags_t[pl.ds(n, 1), :] = bags_p[px * GY + py]
    lane = lax.broadcasted_iota(jnp.int32, (CAP, PEERS), 1)
    for t in range(TABLES):
        line = jnp.zeros((CAP, PEERS), jnp.int32)
        for j in range(8):
            part = bags_t[pl.ds(j, 16, stride=8), :]
            moved = pltpu.roll(part, (j * CAP - t * CAP) % PEERS, axis=1)
            line = jnp.where(lane // CAP == j, moved, line)
        lanes[t] = line

    small[3].wait()
    drain(hot_in, h_rsem.at[3])
    hot_send(hot_in, hot_pin, 4, partner)
    hot_send(hot_s2, hot_ps, 5, partner)

    drain(hot_pin, h_rsem.at[4])
    drain(hot_ps, h_rsem.at[5])
    hot_all[core, block] = hot_s2[...]
    hot_all[other, block] = hot_ps[...]
    for b in range(1, 16):
        from_b = lax.rem(z + 4 - b // 4, 4) * 4 + lax.rem(y + 4 - b % 4, 4)
        hot_all[core, from_b] = hot_in[b - 1]
        hot_all[other, from_b] = hot_pin[b - 1]
    spot = lax.broadcasted_iota(jnp.int32, (HOT, BATCH_DEV), 0)
    sample = lax.broadcasted_iota(jnp.int32, (BATCH_DEV, 2 * PEERS), 0)
    parts = []
    for t in range(TABLES):
        counts = jnp.zeros((HOT, BATCH_DEV), jnp.float32)
        for k in range(HOT_BAG):
            ids = hot_ids_v[pl.ds(t * HOT_BAG + k, 1), :]
            counts = counts + jnp.where(ids == spot, 1.0, 0.0)
        counts = counts.T.astype(jnp.bfloat16)
        high, low = split_bf16(hot_all[t].reshape(HOT, DIM))
        both = jnp.concatenate([high, low], axis=1)
        parts.append(jnp.dot(counts, both, preferred_element_type=jnp.float32))

    for q in range(8):
        drain(rbuf.at[pl.ds(q * 16, 16 if q < 7 else 15)], row_rsem.at[q])
        for t in range(TABLES):
            wanted = jnp.concatenate(
                [lanes[t, pl.ds(2 * q, 1), :], lanes[t, pl.ds(2 * q + 1, 1), :]], axis=1
            )
            onehot = jnp.where(wanted == sample, 1.0, 0.0).astype(jnp.bfloat16)
            rows = rbuf[pl.ds(q * 16, 16), pl.ds(t * CAP, CAP), :].reshape(256, DIM)
            high, low = split_bf16(rows)
            both = jnp.concatenate([high, low], axis=1)
            parts[t] = parts[t] + jnp.dot(onehot, both, preferred_element_type=jnp.float32)
    for t in range(TABLES):
        out_ref[pl.ds(t, BATCH_DEV, stride=2), :] = parts[t][:, :DIM] + parts[t][:, DIM:]

    drain(idx_out.at[pl.ds(0, 4 * (GROUP - 1))], idx_ssem1)
    drain(idx_far, idx_ssem2)
    drain(idx_out.at[pl.ds(0, len(LINE + NEAR))], idx_csem)
    drain(sbuf.at[pl.ds(0, PEERS - 1)], row_ssem)
    for stage, ref in enumerate((hot_r0, hot_r1, hot_r2, hot_in, hot_pin, hot_ps)):
        drain(ref, h_ssem.at[stage])


def body(tables, cold_rows, cold_bags, hot_rows, hot_ids):
    tab = tables.reshape(TABLES * ROWS_DEV, 1, DIM)
    rows = cold_rows[0].transpose(0, 2, 1).reshape(SLOTS, PEERS)
    bags = cold_bags[0].transpose(0, 2, 1).reshape(SLOTS, PEERS)
    ids = hot_ids.transpose(1, 2, 0).reshape(TABLES * HOT_BAG, BATCH_DEV)
    f32, i32 = jnp.float32, jnp.int32
    out = pl.pallas_call(
        kernel,
        out_shape=jax.ShapeDtypeStruct((BATCH_DEV * TABLES, DIM), f32),
        in_specs=[pl.BlockSpec(memory_space=HBM)] * 5,
        out_specs=pl.BlockSpec(memory_space=pltpu.VMEM),
        scratch_shapes=[
            pltpu.VMEM((TABLES * ROWS_DEV + 1, 1, DIM), f32),
            pltpu.VMEM((SLOTS, PEERS), i32),
            pltpu.VMEM((SLOTS, PEERS), i32),
            pltpu.VMEM((TABLES, HOT), i32),
            pltpu.VMEM((TABLES, HOT), i32),
            pltpu.SMEM((TABLES, HOT), i32),
            pltpu.VMEM((TABLES * HOT_BAG, BATCH_DEV), i32),
            pltpu.VMEM((PEERS, PEERS), i32),
            pltpu.VMEM((PEERS, 1, PEERS), i32),
            pltpu.VMEM((4, GROUP, 1, PEERS), i32),
            pltpu.SMEM((len(LINE), 1, PEERS), i32),
            pltpu.SMEM((len(NEAR), 1, PEERS), i32),
            pltpu.SMEM((3, GROUP, 1, PEERS), i32),
            pltpu.SMEM((GROUP, 1, PEERS), i32),
            pltpu.VMEM((PEERS, PEERS), i32),
            pltpu.VMEM((PEERS, 1, PEERS), i32),
            pltpu.VMEM((TABLES, CAP, PEERS), i32),
            pltpu.VMEM((PEERS, SLOTS, DIM), f32),
            pltpu.VMEM((PEERS, SLOTS, DIM), f32),
            pltpu.VMEM((TABLES, 16, 16, DIM), f32),
            pltpu.VMEM((16, 16, DIM), f32),
            pltpu.VMEM((16, 16, DIM), f32),
            pltpu.VMEM((16, 16, DIM), f32),
            pltpu.VMEM((16, DIM), f32),
            pltpu.VMEM((3, 16, DIM), f32),
            pltpu.VMEM((16, DIM), f32),
            pltpu.VMEM((15, 16, DIM), f32),
            pltpu.VMEM((15, 16, DIM), f32),
            pltpu.VMEM((16, DIM), f32),
            pltpu.VMEM((TABLES, 16, 16, DIM), f32),
            pltpu.SemaphoreType.DMA,
            pltpu.SemaphoreType.DMA((4,)),
            pltpu.SemaphoreType.DMA,
            pltpu.SemaphoreType.DMA,
            pltpu.SemaphoreType.DMA,
            pltpu.SemaphoreType.DMA,
            pltpu.SemaphoreType.DMA,
            pltpu.SemaphoreType.DMA,
            pltpu.SemaphoreType.DMA((2,)),
            pltpu.SemaphoreType.DMA,
            pltpu.SemaphoreType.DMA,
            pltpu.SemaphoreType.DMA((8,)),
            pltpu.SemaphoreType.DMA((6,)),
            pltpu.SemaphoreType.DMA((6,)),
        ],
        compiler_params=pltpu.CompilerParams(
            collective_id=0, has_side_effects=True, vmem_limit_bytes=48 << 20
        ),
    )(tab, *(pltpu.with_memory_space_constraint(a, HBM) for a in (rows, bags, hot_rows, ids)))
    return out.reshape(BATCH_DEV, TABLES, DIM)


def solution(mesh):
    both = ("gx", "gy")
    return jax.shard_map(
        body,
        mesh=mesh,
        in_specs=(
            P(None, both, None),
            P(both, None, None, None),
            P(both, None, None, None),
            P(),
            P(both, None, None),
        ),
        out_specs=P(both, None, None),
        check_vma=False,
    )
```
